512 devices in a mesh: depth: 16 (over z), tx: 8 (over x, core), ty: 4 (over y).
Axes of the slice: x: 4, y: 4, z: 16, core: 2. Of those that a mesh axis runs over, the one named last changes fastest.
Arguments:
- slices: float32 [16, 2, 2048, 1024], P('depth', None, 'tx', 'ty'), may hold values from -1.15 to 1.15
- thickness: float32 [16], P('depth'), may hold values from 0.1 to 0.6
- probes: float32 [8, 2, 128, 128], replicated, may hold values from -4 to 4
- centers: int32 [8, 4, 12, 2], P('tx', 'ty'), may hold values from 0 to 255
- batch_of: int32 [8, 4, 12, 1], P('tx', 'ty'), may hold values from 0 to 7; in each aligned block of 12 rows (0 to 11, 12 to 23, ..., all dimensions but the last counted through in order) at most 2 rows name the same one
- intensity: float32 [8, 4, 12, 128, 128], P('tx', 'ty'), may hold values from 0 to 2
Outputs:
- gradient: float32 [16, 2, 2048, 1024], P('depth', None, 'tx', 'ty')
The draws below stay inside these ranges and needn't reach their ends.
Inputs may be any that keep to these rules, and one draw needn't show every extreme that they name: `batch_of`: among the windows of one tile, no micro-batch appears more than 2 times.
All inputs are finite; a program needn't handle non-finite values.
Results may differ from the reference program's by a relative error of at most 0.0003.
Values sent between devices are 32-bit elements; how exact they have to be, the bound alone decides.
A program may use at most 64 MiB of HBM per device.

```python
import math
import jax
import jax.numpy as jnp
import numpy as np
from jax import lax

WINDOW = 128
HALF = 64
TILE = 256
MB = 8
CAP = 2
WIN = 12
SLICES = 16
NX = 2048
NY = 1024
N_TX = 8
N_TY = 4


def draw_slices(key, part):
    first_key, second_key = jax.random.split(jax.random.fold_in(key, 11))
    shape = (SLICES, NX, NY)
    magnitude = jax.random.uniform(first_key, shape, jnp.float32, 0.9, 1.1)
    phases = jax.random.uniform(second_key, shape, jnp.float32, -0.6, 0.6)
    return jnp.stack([magnitude * jnp.cos(phases), magnitude * jnp.sin(phases)], axis=1)


def touch_ends(drawn, stream_key, low, largest):
    spot = [jax.random.randint(jax.random.fold_in(stream_key, axis), (), 0, length) for axis, length in enumerate(drawn.shape)]
    longest = drawn.shape.index(max(drawn.shape))
    next_to = spot[:longest] + [(spot[longest] + 1) % drawn.shape[longest]] + spot[longest + 1:]
    return drawn.at[tuple(spot)].set(low).at[tuple(next_to)].set(largest)


def block_levels(rng, shape, pieces, least, largest):
    def one(position, shards_of):
        heights = jax.random.uniform(jax.random.fold_in(jax.random.fold_in(rng, 6), position), (shards_of,), jnp.float32, least / len(pieces), largest / len(pieces))
        return jnp.repeat(jnp.exp(heights), shape[position] // shards_of).reshape((-1,) + (1,) * (len(shape) - position - 1))

    loudness = one(*pieces[0])
    for cut in pieces[1:]:
        loudness = loudness * one(*cut)
    return loudness


def shared_out(own_key, own, number, rows, number_of, top, bound, slope):
    sequence = jax.random.permutation(own_key, number_of)
    crowded, ordinary = load_shares(number_of, rows * top, bound, slope, True), load_shares(number_of, rows * top, bound, slope, False)
    places = jnp.arange(number_of)

    def named(sizes, turn):
        used = int((sizes > 0).sum())
        fixed = max(1, used // 4)
        moved = fixed + (places - fixed + turn * (used - fixed)) % max(1, number_of - fixed)
        return jnp.zeros((number_of,), jnp.int32).at[sequence[jnp.where(places < fixed, places, moved)]].set(jnp.asarray(sizes, jnp.int32))

    sizes = jnp.where(number % 4 == 0, named(crowded, number // 4), named(ordinary, number - number // 4 - 1))
    mixed = jax.random.permutation(jax.random.fold_in(own, 3), number_of)
    donor, taker = mixed[0:number_of // 2 * 2:2], mixed[1:number_of // 2 * 2:2]
    margin = jnp.minimum(sizes[donor] - 1, bound - sizes[taker]) // 2
    margin = jnp.where((donor == sequence[0]) | (taker == sequence[0]) | (sizes[taker] == 0), 0, jnp.maximum(margin, 0))
    moved = jax.random.randint(jax.random.fold_in(own, 4), (number_of // 2,), 0, 1 << 20) % (margin + 1)
    sizes = sizes.at[donor].add(-moved).at[taker].add(moved)
    labels = jnp.searchsorted(jnp.cumsum(sizes), jnp.arange(rows * top), side="right").astype(jnp.int32)
    listing = labels.reshape(top, rows).T
    listing = listing[jax.random.permutation(jax.random.fold_in(own, 1), rows)]
    turn = jax.random.randint(jax.random.fold_in(own, 2), (rows, 1), 0, top)
    return jnp.take_along_axis(listing, (jnp.arange(top)[None, :] + turn) % top, axis=1)


def load_shares(number_of, total, limit, lean, full):
    loads = [(1 << 20) // math.isqrt(grade ** lean) + 1 for grade in range(1, number_of + 1)]
    largest = limit if full else min(limit, max(-(-total // number_of), total * loads[0] // sum(loads)))
    least = 1 if total - largest >= number_of - 1 else 0
    holding, rest = [largest] + [least] * (number_of - 1), total - largest - least * (number_of - 1)
    while rest > 0:
        free = [i for i in range(1, number_of) if holding[i] < largest] or [i for i in range(1, number_of) if holding[i] < limit]
        whole, left = sum([loads[i] for i in free]), rest
        for i in free:
            more = min(limit - holding[i], max(1, left * loads[i] // whole), rest)
            holding[i] = holding[i] + more
            rest = rest - more
    return np.array(holding)


def normal_values(key, dims, spread, reach, held_as=jnp.bfloat16):
    entries = spread * jax.random.normal(key, dims, jnp.float32)
    return jnp.clip(entries, min=-reach, max=reach).astype(held_as)


def setup_inputs(seed: int = 0) -> dict:
    seeds = jax.random.split(jax.random.key(seed), 7)
    slices = draw_slices(jax.random.fold_in(seeds[6], 71), 0)
    thickness = jnp.clip(jnp.exp(math.log(0.6) - 1.7917595 * jax.random.uniform(seeds[1], (SLICES,), jnp.float32) ** block_levels(seeds[1], (SLICES,), ((0, 16),), -0.2, 0.2)), 0.1, 0.6)
    probes = normal_values(seeds[2], (MB, 2, WINDOW, WINDOW), 0.7, 4.0, jnp.float32)
    centers = touch_ends(jax.random.randint(seeds[3], (N_TX, N_TY, WIN, 2), 0, TILE), jax.random.fold_in(seeds[3], 1), 0, TILE - 1).astype(jnp.int32)
    batch_of_keys = jax.random.split(jax.random.fold_in(seeds[4], 1), N_TX * N_TY * WIN // WIN)
    batch_of_turns = jax.random.permutation(jax.random.fold_in(seeds[4], 3), N_TX * N_TY * WIN // WIN)
    batch_of = jax.vmap(lambda own, number: shared_out(jax.random.fold_in(seeds[4], 2), own, number, WIN, MB, 1, CAP, 2))(batch_of_keys, batch_of_turns).reshape((N_TX, N_TY, WIN, 1))
    intensity = jnp.clip(2.0 * jax.random.uniform(seeds[5], (N_TX, N_TY, WIN, WINDOW, WINDOW), jnp.float32) ** block_levels(seeds[5], (N_TX, N_TY, WIN, WINDOW, WINDOW), ((0, 8), (1, 4)), -0.2, 0.2), 0.0, 2.0)
    return {"slices": slices, "thickness": thickness, "probes": probes, "centers": centers, "batch_of": batch_of, "intensity": intensity}


def kernel_planes(thick):
    counts = jnp.arange(WINDOW, dtype=jnp.int32)
    offset = (counts + HALF) % WINDOW - HALF
    squares = offset[:, None] * offset[:, None] + offset[None, :] * offset[None, :]
    phases = thick * (squares.astype(jnp.float32) * (math.pi / (HALF * HALF)))
    return jnp.cos(phases), jnp.sin(phases)


def transform(values):
    return jnp.fft.fft2(values, norm="ortho")


def inverse(values):
    return jnp.fft.ifft2(values, norm="ortho")


def window_terms(illumination, patches, kernels, target):
    def forward(carried, inputs):
        patch_now, kernel_now = inputs
        incident = inverse(kernel_now * transform(carried))
        return incident * patch_now, incident

    leaving, incidents = lax.scan(forward, illumination, (patches, kernels))
    detector = transform(leaving)
    residue = 2.0 * (jnp.real(detector) ** 2 + jnp.imag(detector) ** 2 - target) * detector

    def backward(returning, inputs):
        patch_now, kernel_now, incident = inputs
        slice_term = jnp.conj(incident) * returning
        returning = inverse(jnp.conj(kernel_now) * transform(jnp.conj(patch_now) * returning))
        return returning, slice_term

    _, slice_terms = lax.scan(backward, inverse(residue), (patches, kernels, incidents), reverse=True)
    return slice_terms


def reference(slices, thickness, probes, centers, batch_of, intensity):
    field = slices[:, 0] + 1j * slices[:, 1]
    padded = jnp.pad(field, ((0, 0), (HALF, HALF), (HALF, HALF)), mode="wrap")
    cosines, sines = jax.vmap(kernel_planes)(thickness)
    kernels = cosines - 1j * sines
    illuminations = probes[:, 0] + 1j * probes[:, 1]
    zero_index = jnp.int32(0)

    def per_tile(tile_index, accumulated):
        tile_row = (tile_index // N_TY).astype(jnp.int32)
        tile_col = (tile_index % N_TY).astype(jnp.int32)
        centre_table = centers[tile_row, tile_col]
        start_rows = (tile_row * TILE + centre_table[:, 0]).astype(jnp.int32)
        start_cols = (tile_col * TILE + centre_table[:, 1]).astype(jnp.int32)

        def cut_window(start_row, start_col):
            return lax.dynamic_slice(padded, (zero_index, start_row, start_col), (SLICES, WINDOW, WINDOW))

        patches = jax.vmap(cut_window)(start_rows, start_cols)
        chosen = illuminations[batch_of[tile_row, tile_col, :, 0]]
        slice_terms = jax.vmap(window_terms, in_axes=(0, 0, None, 0))(chosen, patches, kernels, intensity[tile_row, tile_col])

        def place(which, accumulated):
            start_row = start_rows[which]
            start_col = start_cols[which]
            current = lax.dynamic_slice(accumulated, (zero_index, start_row, start_col), (SLICES, WINDOW, WINDOW))
            return lax.dynamic_update_slice(accumulated, current + slice_terms[which], (zero_index, start_row, start_col))

        return lax.fori_loop(0, WIN, place, accumulated)

    accumulated = lax.fori_loop(0, N_TX * N_TY, per_tile, jnp.zeros(padded.shape, padded.dtype))
    folded_rows = accumulated[:, HALF:HALF + NX, :]
    folded_rows = folded_rows.at[:, :HALF].add(accumulated[:, HALF + NX:, :])
    folded_rows = folded_rows.at[:, NX - HALF:].add(accumulated[:, :HALF, :])
    folded = folded_rows[:, :, HALF:HALF + NY]
    folded = folded.at[:, :, :HALF].add(folded_rows[:, :, HALF + NY:])
    folded = folded.at[:, :, NY - HALF:].add(folded_rows[:, :, :HALF])
    return jnp.stack([jnp.real(folded), jnp.imag(folded)], axis=1)
```

```python
import functools
import math

import jax
import jax.numpy as jnp
from jax import lax
from jax.experimental import pallas as pl
from jax.experimental.pallas import tpu as pltpu
from jax.sharding import PartitionSpec as P

GROUP = 2
LAG_NUM, LAG_DEN = 9, 5
STAGGER = 1400
MESH = pl.DeviceIdType.MESH
F32 = jnp.float32
BF16 = jnp.bfloat16


def padded_2(block, sides, width):
    for axis, dim in sides:
        count = lax.axis_size(axis)
        forward = [(i, (i + 1) % count) for i in range(count)]
        backward = [(target, source) for source, target in forward]
        low = lax.ppermute(
            lax.slice_in_dim(block, block.shape[dim] - width, None, axis=dim), axis, forward
        )
        high = lax.ppermute(lax.slice_in_dim(block, 0, width, axis=dim), axis, backward)
        block = jnp.concatenate([low, block, high], axis=dim)
    return block


def split(values):
    high = values.astype(BF16)
    return high, (values - high.astype(F32)).astype(BF16)


def times(wave, high_table, low_table):
    high, low = split(wave)
    total = jnp.dot(high, low_table, preferred_element_type=F32)
    total += jnp.dot(low, high_table, preferred_element_type=F32)
    return total + jnp.dot(high, high_table, preferred_element_type=F32)


def turned(wave):
    n = wave.shape[0]
    return jnp.concatenate([wave[:, :n].T, wave[:, n:].T], axis=1)


def both_sides(wave, high_table, low_table):
    return times(turned(times(wave, high_table, low_table)), high_table, low_table)


def multiply(first, second):
    n = first.shape[0]
    a, b, c, d = first[:, :n], first[:, n:], second[:, :n], second[:, n:]
    return jnp.concatenate([a * c - b * d, a * d + b * c], axis=1)


def conj_multiply(first, second):
    n = first.shape[0]
    a, b, c, d = first[:, :n], first[:, n:], second[:, :n], second[:, n:]
    return jnp.concatenate([a * c + b * d, a * d - b * c], axis=1)


def keep_table(real, imag, at, high_ref, low_ref):
    n = real.shape[0]
    (rh, rl), (ih, il) = split(real), split(imag)
    for ref, r, m in ((high_ref, rh, ih), (low_ref, rl, il)):
        ref[at, 0:n, 0:n] = r
        ref[at, 0:n, n : 2 * n] = m
        ref[at, n : 2 * n, 0:n] = -m
        ref[at, n : 2 * n, n : 2 * n] = r


def gather(centers, owners, padded, probes, cuts, starts):
    windows, n = cuts.shape[:2]
    flipped = lax.rem(lax.axis_index("depth"), 2) == 0

    @pl.loop(0, windows)
    def _(w):
        row, col = centers[w, 0], centers[w, 1]
        row_in, col_in = lax.rem(row, 8), lax.rem(col, 128)
        rows = pl.ds(pl.multiple_of(row - row_in, 8), n + 8)
        cols = pl.ds(pl.multiple_of(col - col_in, 128), 2 * n)
        planes = []
        for plane in range(2):
            block = padded[plane, rows, cols]
            block = pltpu.roll(block, lax.rem(2 * n - col_in, 2 * n), 1)[:, :n]
            planes.append(pltpu.roll(block, lax.rem(n + 8 - row_in, n + 8), 0)[:n])

        @pl.when(flipped)
        def _():
            cuts[w] = jnp.concatenate([planes[0].T, planes[1].T], axis=1)

        @pl.when(jnp.logical_not(flipped))
        def _():
            cuts[w] = jnp.concatenate(planes, axis=1)

        probe = probes[owners[w, 0]]
        starts[w] = jnp.concatenate([probe[0], probe[1]], axis=1)


def chain(
    windows, group, groups,
    phase, tables, cut, starts, measured,
    terms,
    phases, forth_high, forth_low, back_high, back_low,
    patches, psis, waves_in, waves_out, turns_in, turns_out, landed,
    phase_sent, phase_got, cut_sent, patch_got, wave_sent, wave_got, turn_sent, turn_got,
    term_sent, term_got,
):
    n = tables.shape[0]
    place = lax.axis_index("depth")
    mine = lax.rem(place, group)
    stage = lax.div(place, group)
    last = groups - 1
    count = lax.div(windows - mine + group - 1, group)

    def send(src, dst, sent, got, target):
        return pltpu.make_async_remote_copy(
            src_ref=src, dst_ref=dst, send_sem=sent, recv_sem=got,
            device_id={"depth": target}, device_id_type=MESH,
        )

    def beside(step):
        return stage * group + lax.rem(mine + step, group)

    barrier = pltpu.get_barrier_semaphore()
    for step in range(1, group):
        pl.semaphore_signal(barrier, inc=1, device_id={"depth": beside(step)}, device_id_type=MESH)

    @pl.when(stage > 0)
    def _():
        pl.semaphore_signal(barrier, inc=1, device_id={"depth": place - group}, device_id_type=MESH)

    @pl.when(stage < last)
    def _():
        pl.semaphore_signal(barrier, inc=1, device_id={"depth": place + group}, device_id_type=MESH)

    inner = jnp.where(stage > 0, 1, 0) + jnp.where(stage < last, 1, 0)
    pl.semaphore_wait(barrier, group - 1 + inner)

    for step in range(1, group):
        send(phase, phases.at[mine], phase_sent.at[step], phase_got.at[mine], beside(step)).start()

    def patch_copy(w):
        which = lax.div(w, group)
        to = lax.rem(w, group)
        return send(
            cut.at[w], patches.at[which, mine], cut_sent.at[w], patch_got.at[which, mine],
            stage * group + to,
        )

    @pl.loop(0, windows)
    def _(w):
        to = lax.rem(w, group)

        @pl.when(to != mine)
        def _():
            patch_copy(w).start()

        @pl.when(to == mine)
        def _():
            patches[lax.div(w, group), mine] = cut[w]

    cosine, sine = tables[:, :n], tables[:, n:]
    keep_table(cosine, -sine, group, forth_high, forth_low)
    keep_table(cosine, sine, group, back_high, back_low)
    phases[mine] = phase[...]
    for step in range(1, group):
        other = lax.rem(mine + step, group)
        send(phase, phases.at[other], phase_sent.at[step], phase_got.at[other], beside(step)).wait_recv()

    @pl.loop(0, group)
    def _(r):
        turn = phases[r]
        real, imag = turn[0:1, :n], turn[0:1, n:]
        scaled = jnp.concatenate([cosine * real - sine * imag, cosine * imag + sine * real], axis=1)
        table = times(scaled, forth_high[group], forth_low[group])
        keep_table(table[:, :n], table[:, n:], r, forth_high, forth_low)
        keep_table(table[:, :n], -table[:, n:], r, back_high, back_low)

    def wave_copy(j):
        return send(waves_out.at[j], waves_in.at[j], wave_sent.at[j], wave_got.at[j], place + group)

    def turn_copy(j):
        return send(turns_out.at[j], turns_in.at[j], turn_sent.at[j], turn_got.at[j], place - group)

    def term_copy(j, r):
        return send(
            psis.at[j, r], landed.at[j * group + mine], term_sent.at[j, r],
            term_got.at[j * group + mine], stage * group + r,
        )

    if STAGGER:
        shared = 2 * mine + lax.rem(lax.axis_index("tx"), 2)
        for turn in range(1, 2 * group):

            @pl.when((stage == 0) & (shared == turn))
            def _():
                pl.delay(turn * STAGGER)

    def go(j):
        @pl.when(stage == 0)
        def _():
            waves_in[j] = starts[j * group + mine]

        @pl.when(stage > 0)
        def _():
            wave_copy(j).wait_recv()

        wave = waves_in[j]
        for r in range(group):
            psi = both_sides(wave, forth_high[r], forth_low[r])
            psis[j, r] = psi

            @pl.when(mine != r)
            def _():
                send(
                    cut.at[0], patches.at[j, r], cut_sent.at[0], patch_got.at[j, r], stage * group + r
                ).wait_recv()

            wave = multiply(psi, patches[j, r])

        @pl.when(stage < last)
        def _():
            waves_out[j] = wave
            wave_copy(j).start()

        @pl.when(stage == last)
        def _():
            far = both_sides(wave, forth_high[group], forth_low[group])
            real, imag = far[:, :n], far[:, n:]
            target = measured[j * group + mine].T
            excess = 2.0 * (real * real + imag * imag - target)
            chi = jnp.concatenate([excess * real, excess * imag], axis=1)
            turns_in[j] = both_sides(chi, back_high[group], back_low[group])

    def come_back(j):
        @pl.when(stage < last)
        def _():
            turn_copy(j).wait_recv()

        wave = turns_in[j]
        for r in reversed(range(group)):
            term = conj_multiply(psis[j, r], wave)
            if r % 2 == 0:
                term = turned(term)

            @pl.when(mine == r)
            def _():
                landed[j * group + mine] = term

            @pl.when(mine != r)
            def _():
                psis[j, r] = term
                term_copy(j, r).start()

            wave = both_sides(conj_multiply(patches[j, r], wave), back_high[r], back_low[r])

        @pl.when(stage > 0)
        def _():
            turns_out[j] = wave
            turn_copy(j).start()

    lag = jnp.minimum(count, lax.div((last - stage) * LAG_NUM, LAG_DEN))

    @pl.loop(0, count + lag)
    def _(t):
        @pl.when(t < count)
        def _():
            go(t)

        @pl.when(t >= lag)
        def _():
            come_back(t - lag)

    for step in range(1, group):
        send(phase, phases.at[mine], phase_sent.at[step], phase_got.at[mine], beside(step)).wait_send()

    @pl.loop(0, windows)
    def _(w):
        @pl.when(lax.rem(w, group) != mine)
        def _():
            patch_copy(w).wait_send()
            send(
                psis.at[0, 0], landed.at[w], term_sent.at[0, 0], term_got.at[w], beside(1)
            ).wait_recv()

    @pl.loop(0, count)
    def _(j):
        @pl.when(stage < last)
        def _():
            wave_copy(j).wait_send()

        @pl.when(stage > 0)
        def _():
            turn_copy(j).wait_send()

        for r in range(group):

            @pl.when(mine != r)
            def _():
                term_copy(j, r).wait_send()

    @pl.loop(0, windows)
    def _(w):
        terms[w] = landed[w]


def spread(centers, terms, total):
    windows, n = terms.shape[0], terms.shape[1]
    total[...] = jnp.zeros(total.shape, F32)

    @pl.loop(0, windows)
    def _(w):
        row, col = centers[w, 0], centers[w, 1]
        row_in, col_in = lax.rem(row, 8), lax.rem(col, 128)
        rows = pl.ds(pl.multiple_of(row - row_in, 8), n + 8)
        cols = pl.ds(pl.multiple_of(col - col_in, 128), 2 * n)
        term = terms[w]
        for plane in range(2):
            block = term[:, plane * n : (plane + 1) * n]
            block = jnp.concatenate([block, jnp.zeros((8, n), F32)], axis=0)
            block = pltpu.roll(block, row_in, 0)
            block = jnp.concatenate([block, jnp.zeros((n + 8, n), F32)], axis=1)
            total[plane, rows, cols] += pltpu.roll(block, col_in, 1)


def local(slices, thickness, probes, centers, batch_of, intensity):
    sections = lax.axis_size("depth")
    n = probes.shape[-1]
    half = n // 2
    centre_table, owners, measured = centers[0, 0], batch_of[0, 0], intensity[0, 0]
    windows = owners.shape[0]
    group, groups = GROUP, sections // GROUP
    most = -(-windows // group)

    padded = padded_2(slices[0], (("tx", 1), ("ty", 2)), half)
    side_rows, side_cols = padded.shape[1:]
    counts = jnp.arange(n, dtype=jnp.int32)
    angles = (counts[:, None] * counts[None, :] % n).astype(F32) * (2.0 * math.pi / n)
    tables = jnp.concatenate([jnp.cos(angles), jnp.sin(angles)], axis=1) * (1.0 / math.sqrt(n))
    offset = (counts + half) % n - half
    turn = thickness[0] * ((offset * offset).astype(F32) * (math.pi / (half * half)))
    phase = jnp.broadcast_to(jnp.concatenate([jnp.cos(turn), -jnp.sin(turn)])[None], (8, 2 * n))

    smem = pl.BlockSpec(memory_space=pltpu.SMEM)
    vmem = pl.BlockSpec(memory_space=pltpu.VMEM)
    page = (n, 2 * n)
    dma = pltpu.SemaphoreType.DMA
    cuts, starts = pl.pallas_call(
        gather,
        name="gather",
        out_shape=[jax.ShapeDtypeStruct((windows, *page), F32)] * 2,
        in_specs=[smem, smem, vmem, vmem],
        out_specs=[vmem, vmem],
    )(centre_table, owners, padded, probes)

    terms = pl.pallas_call(
        functools.partial(chain, windows, group, groups),
        name="chain",
        out_shape=jax.ShapeDtypeStruct((windows, *page), F32),
        in_specs=[vmem, vmem, vmem, vmem, vmem],
        out_specs=vmem,
        scratch_shapes=[
            pltpu.VMEM((group, 8, 2 * n), F32),
            pltpu.VMEM((group + 1, 2 * n, 2 * n), BF16),
            pltpu.VMEM((group + 1, 2 * n, 2 * n), BF16),
            pltpu.VMEM((group + 1, 2 * n, 2 * n), BF16),
            pltpu.VMEM((group + 1, 2 * n, 2 * n), BF16),
            pltpu.VMEM((most, group, *page), F32),
            pltpu.VMEM((most, group, *page), F32),
            pltpu.VMEM((most, *page), F32),
            pltpu.VMEM((most, *page), F32),
            pltpu.VMEM((most, *page), F32),
            pltpu.VMEM((most, *page), F32),
            pltpu.VMEM((windows, *page), F32),
            dma((group,)),
            dma((group,)),
            dma((windows,)),
            dma((most, group)),
            dma((most,)),
            dma((most,)),
            dma((most,)),
            dma((most,)),
            dma((most, group)),
            dma((windows,)),
        ],
        compiler_params=pltpu.CompilerParams(collective_id=0, has_side_effects=True),
    )(phase, tables, cuts, starts, measured)

    gradient_pad = pl.pallas_call(
        spread,
        name="spread",
        out_shape=jax.ShapeDtypeStruct((2, side_rows, side_cols), F32),
        in_specs=[smem, vmem],
        out_specs=vmem,
    )(centre_table, terms)

    row_rims = jnp.concatenate([gradient_pad[:, :half], gradient_pad[:, -half:]], axis=1)
    beside_all = padded_2(row_rims, (("tx", 1),), half)
    inner = gradient_pad[:, half:-half]
    inner = inner.at[:, :half].add(beside_all[:, :half])
    inner = inner.at[:, -half:].add(beside_all[:, -half:])
    col_rims = jnp.concatenate([inner[:, :, :half], inner[:, :, -half:]], axis=2)
    beside = padded_2(col_rims, (("ty", 2),), half)
    result = inner[:, :, half:-half]
    result = result.at[:, :, :half].add(beside[:, :, :half])
    result = result.at[:, :, -half:].add(beside[:, :, -half:])
    return result[None]


def solution(mesh):
    placed = (
        P("depth", None, "tx", "ty"),
        P("depth"),
        P(),
        P("tx", "ty", None, None),
        P("tx", "ty", None, None),
        P("tx", "ty", None, None, None),
    )
    return jax.shard_map(
        local, mesh=mesh, in_specs=placed, out_specs=P("depth", None, "tx", "ty"), check_vma=False
    )
```

```python
import functools
import math

import jax
import jax.numpy as jnp
from jax import lax
from jax.experimental import pallas as pl
from jax.experimental.pallas import tpu as pltpu
from jax.sharding import PartitionSpec as P

GROUP = 2
BASE, HOMES = 0, 1
LAG = 13
MESH = pl.DeviceIdType.MESH
F32 = jnp.float32
BF16 = jnp.bfloat16


SIDES = [(dx, dy) for dx in (-1, 0, 1) for dy in (-1, 0, 1) if dx or dy]


def around(dx, dy):
    tx, ty = lax.axis_size("tx"), lax.axis_size("ty")
    return {
        "tx": lax.rem(lax.axis_index("tx") + dx + tx, tx),
        "ty": lax.rem(lax.axis_index("ty") + dy + ty, ty),
    }


def greet_all():
    barrier = pltpu.get_barrier_semaphore()
    for dx, dy in SIDES:
        pl.semaphore_signal(barrier, inc=1, device_id=around(dx, dy), device_id_type=MESH)
    pl.semaphore_wait(barrier, len(SIDES))


def packed(first, second, upper):
    n = first.shape[-1]
    lane = lax.broadcasted_iota(jnp.int32, first.shape, 1)
    keep = lane >= n // 2 if upper else lane < n // 2
    return jnp.where(keep, first, pltpu.roll(second, n // 2, 1))


def exchange(strips, pages, corners, strips_in, pages_in, corners_in, sent, got):
    copies = []
    for k, (dx, dy) in enumerate(SIDES):
        if dy == 0:
            src, dst = strips[dx], strips_in.at[(dx + 1) // 2]
        elif dx == 0:
            src, dst = pages.at[(dy + 1) // 2], pages_in.at[(dy + 1) // 2]
        else:
            at = (dx + 1) + (dy + 1) // 2
            src, dst = corners.at[at], corners_in.at[at]
        copies.append(
            pltpu.make_async_remote_copy(
                src_ref=src, dst_ref=dst, send_sem=sent.at[k], recv_sem=got.at[k],
                device_id=around(dx, dy), device_id_type=MESH,
            )
        )
    return copies


def pack_sides(source, rows, columns, pages, corners):
    for dy in (-1, 1):
        upper, cols = columns[dy]
        first, count = rows[0]
        half = count // 2
        for plane in range(2):
            pages[(dy + 1) // 2, plane] = packed(
                source[plane, first : first + half, cols], source[plane, first + half : first + count, cols], upper
            )
        for dx in (-1, 1):
            first, count = rows[dx]
            corners[(dx + 1) + (dy + 1) // 2] = packed(
                source[0, first : first + count, cols], source[1, first : first + count, cols], upper
            )


def enlarge(tile, padded, pages, corners, strips_in, pages_in, corners_in, sent, got):
    side, n = tile.shape[1], tile.shape[1] // 2
    half = n // 2
    greet_all()
    rows = {-1: (0, half), 0: (0, side), 1: (side - half, half)}
    columns = {-1: (False, slice(0, n)), 1: (True, slice(side - n, side))}
    strips = {-1: tile.at[:, pl.ds(0, half), :], 1: tile.at[:, pl.ds(side - half, half), :]}
    copies = exchange(strips, pages, corners, strips_in, pages_in, corners_in, sent, got)
    for copy, (dx, dy) in zip(copies, SIDES):
        if dy == 0:
            copy.start()
    pack_sides(tile, rows, columns, pages, corners)
    for copy, (dx, dy) in zip(copies, SIDES):
        if dy != 0:
            copy.start()
    padded[:, half : half + side, n : n + side] = tile[...]
    target_rows = {-1: slice(half + side, side + n), 1: slice(0, half)}
    target_cols = {-1: slice(n + side, 2 * n + side), 1: slice(0, n)}
    for copy, (dx, dy) in zip(copies, SIDES):
        copy.wait_recv()
        if dy == 0:
            padded[:, target_rows[dx], n : n + side] = strips_in[(dx + 1) // 2]
        elif dx == 0:
            for plane in range(2):
                page = pages_in[(dy + 1) // 2, plane]
                padded[plane, half : half + n, target_cols[dy]] = page
                padded[plane, half + n : half + side, target_cols[dy]] = pltpu.roll(page, half, 1)
        else:
            corner = corners_in[(dx + 1) + (dy + 1) // 2]
            padded[0, target_rows[dx], target_cols[dy]] = corner
            padded[1, target_rows[dx], target_cols[dy]] = pltpu.roll(corner, half, 1)
    for copy in copies:
        copy.wait_send()


def fold(total, result, pages, corners, strips_in, pages_in, corners_in, sent, got):
    side, n = result.shape[1], result.shape[1] // 2
    half = n // 2
    greet_all()
    rows = {-1: (0, half), 0: (half, side), 1: (half + side, half)}
    columns = {-1: (True, slice(0, n)), 1: (False, slice(n + side, 2 * n + side))}
    mid = pl.ds(n, side)
    strips = {-1: total.at[:, pl.ds(0, half), mid], 1: total.at[:, pl.ds(half + side, half), mid]}
    copies = exchange(strips, pages, corners, strips_in, pages_in, corners_in, sent, got)
    for copy, (dx, dy) in zip(copies, SIDES):
        if dy == 0:
            copy.start()
    pack_sides(total, rows, columns, pages, corners)
    for copy, (dx, dy) in zip(copies, SIDES):
        if dy != 0:
            copy.start()
    result[...] = total[:, half : half + side, n : n + side]
    target_rows = {-1: slice(side - half, side), 1: slice(0, half)}
    target_cols = {-1: slice(side - n, side), 1: slice(0, n)}

    def masked(page, dy):
        lane = lax.broadcasted_iota(jnp.int32, page.shape, 1)
        return jnp.where(lane >= half if dy == -1 else lane < half, page, 0.0)

    for copy, (dx, dy) in zip(copies, SIDES):
        copy.wait_recv()
        if dy == 0:
            result[:, target_rows[dx], :] += strips_in[(dx + 1) // 2]
        elif dx == 0:
            for plane in range(2):
                page = pages_in[(dy + 1) // 2, plane]
                result[plane, 0:n, target_cols[dy]] += masked(page, dy)
                result[plane, n:side, target_cols[dy]] += masked(pltpu.roll(page, half, 1), dy)
        else:
            corner = corners_in[(dx + 1) + (dy + 1) // 2]
            result[0, target_rows[dx], target_cols[dy]] += masked(corner, dy)
            result[1, target_rows[dx], target_cols[dy]] += masked(pltpu.roll(corner, half, 1), dy)
    for copy in copies:
        copy.wait_send()


def split(values):
    high = values.astype(BF16)
    return high, (values - high.astype(F32)).astype(BF16)


def times(wave, high_table, low_table):
    high, low = split(wave)
    total = jnp.dot(high, low_table, preferred_element_type=F32)
    total += jnp.dot(low, high_table, preferred_element_type=F32)
    return total + jnp.dot(high, high_table, preferred_element_type=F32)


def turned(wave):
    n = wave.shape[0]
    return jnp.concatenate([wave[:, :n].T, wave[:, n:].T], axis=1)


def both_sides(wave, high_table, low_table):
    return times(turned(times(wave, high_table, low_table)), high_table, low_table)


def multiply(first, second):
    n = first.shape[0]
    a, b, c, d = first[:, :n], first[:, n:], second[:, :n], second[:, n:]
    return jnp.concatenate([a * c - b * d, a * d + b * c], axis=1)


def conj_multiply(first, second):
    n = first.shape[0]
    a, b, c, d = first[:, :n], first[:, n:], second[:, :n], second[:, n:]
    return jnp.concatenate([a * c + b * d, a * d - b * c], axis=1)


def keep_table(real, imag, at, high_ref, low_ref):
    n = real.shape[0]
    (rh, rl), (ih, il) = split(real), split(imag)
    for ref, r, m in ((high_ref, rh, ih), (low_ref, rl, il)):
        ref[at, 0:n, 0:n] = r
        ref[at, 0:n, n : 2 * n] = m
        ref[at, n : 2 * n, 0:n] = -m
        ref[at, n : 2 * n, n : 2 * n] = r


def gather(centers, owners, padded, probes, cuts, starts):
    windows, n = cuts.shape[:2]
    flipped = lax.rem(lax.axis_index("depth"), 2) == 0

    @pl.loop(0, windows)
    def _(w):
        row, col = centers[0, 0, w, 0], centers[0, 0, w, 1] + n // 2
        row_in, col_in = lax.rem(row, 8), lax.rem(col, 128)
        rows = pl.ds(pl.multiple_of(row - row_in, 8), n + 8)
        cols = pl.ds(pl.multiple_of(col - col_in, 128), 2 * n)
        planes = []
        for plane in range(2):
            block = padded[plane, rows, cols]
            block = pltpu.roll(block, lax.rem(2 * n - col_in, 2 * n), 1)[:, :n]
            planes.append(pltpu.roll(block, lax.rem(n + 8 - row_in, n + 8), 0)[:n])

        @pl.when(flipped)
        def _():
            cuts[w] = jnp.concatenate([planes[0].T, planes[1].T], axis=1)

        @pl.when(jnp.logical_not(flipped))
        def _():
            cuts[w] = jnp.concatenate(planes, axis=1)

        probe = probes[owners[0, 0, w, 0]]
        starts[w] = jnp.concatenate([probe[0], probe[1]], axis=1)


def chain(
    windows, group, groups,
    phase, tables, cut, starts, measured,
    terms,
    phases, forth_high, forth_low, back_high, back_low,
    patches, psis, waves_in, waves_out, turns_in, turns_out, landed,
    phase_sent, phase_got, cut_sent, patch_got, wave_sent, wave_got, turn_sent, turn_got,
    term_sent, term_got,
):
    n = tables.shape[0]
    place = lax.axis_index("depth")
    mine = lax.rem(place, group)
    stage = lax.div(place, group)
    last = groups - 1
    home = mine - BASE
    active = (home >= 0) & (home < HOMES)
    count = jnp.where(active, lax.div(windows - home + HOMES - 1, HOMES), 0)
    before = active & (stage > 0)
    after = active & (stage < last)

    def send(src, dst, sent, got, target):
        return pltpu.make_async_remote_copy(
            src_ref=src, dst_ref=dst, send_sem=sent, recv_sem=got,
            device_id={"depth": target}, device_id_type=MESH,
        )

    def beside(step):
        return stage * group + lax.rem(mine + step, group)

    barrier = pltpu.get_barrier_semaphore()
    for step in range(1, group):
        pl.semaphore_signal(barrier, inc=1, device_id={"depth": beside(step)}, device_id_type=MESH)

    @pl.when(before)
    def _():
        pl.semaphore_signal(barrier, inc=1, device_id={"depth": place - group}, device_id_type=MESH)

    @pl.when(after)
    def _():
        pl.semaphore_signal(barrier, inc=1, device_id={"depth": place + group}, device_id_type=MESH)

    inner = jnp.where(before, 1, 0) + jnp.where(after, 1, 0)
    pl.semaphore_wait(barrier, group - 1 + inner)

    for step in range(1, group):
        send(phase, phases.at[mine], phase_sent.at[step], phase_got.at[mine], beside(step)).start()

    def patch_copy(w):
        which = lax.div(w, HOMES)
        to = BASE + lax.rem(w, HOMES)
        return send(
            cut.at[w], patches.at[which, mine], cut_sent.at[w], patch_got.at[which, mine],
            stage * group + to,
        )

    @pl.loop(0, windows)
    def _(w):
        to = BASE + lax.rem(w, HOMES)

        @pl.when(to != mine)
        def _():
            patch_copy(w).start()

        @pl.when(to == mine)
        def _():
            patches[lax.div(w, HOMES), mine] = cut[w]

    cosine, sine = tables[:, :n], tables[:, n:]
    keep_table(cosine, -sine, group, forth_high, forth_low)
    keep_table(cosine, sine, group, back_high, back_low)
    phases[mine] = phase[...]
    for step in range(1, group):
        other = lax.rem(mine + step, group)
        send(phase, phases.at[other], phase_sent.at[step], phase_got.at[other], beside(step)).wait_recv()

    @pl.loop(0, group)
    def _(r):
        turn = phases[r]
        real, imag = turn[0:1, :n], turn[0:1, n:]
        scaled = jnp.concatenate([cosine * real - sine * imag, cosine * imag + sine * real], axis=1)
        table = times(scaled, forth_high[group], forth_low[group])
        keep_table(table[:, :n], table[:, n:], r, forth_high, forth_low)
        keep_table(table[:, :n], -table[:, n:], r, back_high, back_low)

    def wave_copy(j):
        return send(waves_out.at[j], waves_in.at[j], wave_sent.at[j], wave_got.at[j], place + group)

    def turn_copy(j):
        return send(turns_out.at[j], turns_in.at[j], turn_sent.at[j], turn_got.at[j], place - group)

    def term_copy(j, r):
        return send(
            psis.at[j, r], landed.at[j * HOMES + home], term_sent.at[j, r],
            term_got.at[j * HOMES + home], stage * group + r,
        )

    def go(j):
        @pl.when(stage == 0)
        def _():
            waves_in[j] = starts[j * HOMES + home]

        @pl.when(stage > 0)
        def _():
            wave_copy(j).wait_recv()

        wave = waves_in[j]
        for r in range(group):
            psi = both_sides(wave, forth_high[r], forth_low[r])
            psis[j, r] = psi

            @pl.when(mine != r)
            def _():
                send(
                    cut.at[0], patches.at[j, r], cut_sent.at[0], patch_got.at[j, r], stage * group + r
                ).wait_recv()

            wave = multiply(psi, patches[j, r])

        @pl.when(stage < last)
        def _():
            waves_out[j] = wave
            wave_copy(j).start()

        @pl.when(stage == last)
        def _():
            far = both_sides(wave, forth_high[group], forth_low[group])
            real, imag = far[:, :n], far[:, n:]
            target = measured[j * HOMES + home].T
            excess = 2.0 * (real * real + imag * imag - target)
            chi = jnp.concatenate([excess * real, excess * imag], axis=1)
            turns_in[j] = both_sides(chi, back_high[group], back_low[group])

    def come_back(j):
        @pl.when(stage < last)
        def _():
            turn_copy(j).wait_recv()

        wave = turns_in[j]
        for r in reversed(range(group)):
            term = conj_multiply(psis[j, r], wave)
            if r % 2 == 0:
                term = turned(term)

            @pl.when(mine == r)
            def _():
                landed[j * HOMES + home] = term

            @pl.when(mine != r)
            def _():
                psis[j, r] = term
                term_copy(j, r).start()

            if r > 0:
                wave = both_sides(conj_multiply(patches[j, r], wave), back_high[r], back_low[r])

        @pl.when(stage > 0)
        def _():
            turns_out[j] = both_sides(conj_multiply(patches[j, 0], wave), back_high[0], back_low[0])
            turn_copy(j).start()

    lag = jnp.minimum(count, lax.div((2 * (last - stage) + 1) * LAG, 7 * HOMES))

    @pl.loop(0, count + lag)
    def _(t):
        @pl.when(t < count)
        def _():
            go(t)

        @pl.when(t >= lag)
        def _():
            come_back(t - lag)

    for step in range(1, group):
        send(phase, phases.at[mine], phase_sent.at[step], phase_got.at[mine], beside(step)).wait_send()

    @pl.loop(0, windows)
    def _(w):
        @pl.when(BASE + lax.rem(w, HOMES) != mine)
        def _():
            patch_copy(w).wait_send()
            send(
                psis.at[0, 0], landed.at[w], term_sent.at[0, 0], term_got.at[w], beside(1)
            ).wait_recv()

    @pl.loop(0, count)
    def _(j):
        @pl.when(stage < last)
        def _():
            wave_copy(j).wait_send()

        @pl.when(stage > 0)
        def _():
            turn_copy(j).wait_send()

        for r in range(group):

            @pl.when(mine != r)
            def _():
                term_copy(j, r).wait_send()

    @pl.loop(0, windows)
    def _(w):
        terms[w] = landed[w]


def spread(centers, terms, total):
    windows, n = terms.shape[0], terms.shape[1]
    total[...] = jnp.zeros(total.shape, F32)

    @pl.loop(0, windows)
    def _(w):
        row, col = centers[0, 0, w, 0], centers[0, 0, w, 1] + n // 2
        row_in, col_in = lax.rem(row, 8), lax.rem(col, 128)
        rows = pl.ds(pl.multiple_of(row - row_in, 8), n + 8)
        cols = pl.ds(pl.multiple_of(col - col_in, 128), 2 * n)
        term = terms[w]
        for plane in range(2):
            block = term[:, plane * n : (plane + 1) * n]
            block = jnp.concatenate([block, jnp.zeros((8, n), F32)], axis=0)
            block = pltpu.roll(block, row_in, 0)
            block = jnp.concatenate([block, jnp.zeros((n + 8, n), F32)], axis=1)
            total[plane, rows, cols] += pltpu.roll(block, col_in, 1)


def local(slices, thickness, probes, centers, batch_of, intensity):
    sections = lax.axis_size("depth")
    n = probes.shape[-1]
    half = n // 2
    measured = intensity[0, 0]
    windows = measured.shape[0]
    group, groups = GROUP, sections // GROUP
    most = -(-windows // HOMES)

    counts = jnp.arange(n, dtype=jnp.int32)
    angles = (counts[:, None] * counts[None, :] % n).astype(F32) * (2.0 * math.pi / n)
    tables = jnp.concatenate([jnp.cos(angles), jnp.sin(angles)], axis=1) * (1.0 / math.sqrt(n))
    offset = (counts + half) % n - half
    turn = thickness[0] * ((offset * offset).astype(F32) * (math.pi / (half * half)))
    phase = jnp.broadcast_to(jnp.concatenate([jnp.cos(turn), -jnp.sin(turn)])[None], (8, 2 * n))

    smem = pl.BlockSpec(memory_space=pltpu.SMEM)
    vmem = pl.BlockSpec(memory_space=pltpu.VMEM)
    page = (n, 2 * n)
    dma = pltpu.SemaphoreType.DMA
    side = slices.shape[2]
    tile_shape = jax.ShapeDtypeStruct((2, side, side), F32)
    wide_shape = jax.ShapeDtypeStruct((2, side + n, side + 2 * n), F32)
    edges = [
        pltpu.VMEM((2, 2, n, n), F32),
        pltpu.VMEM((4, half, n), F32),
        pltpu.VMEM((2, 2, half, side), F32),
        pltpu.VMEM((2, 2, n, n), F32),
        pltpu.VMEM((4, half, n), F32),
        dma((len(SIDES),)),
        dma((len(SIDES),)),
    ]
    padded = pl.pallas_call(
        enlarge,
        name="enlarge",
        out_shape=wide_shape,
        in_specs=[vmem],
        out_specs=vmem,
        scratch_shapes=edges,
        compiler_params=pltpu.CompilerParams(collective_id=1, has_side_effects=True),
    )(slices[0])

    cuts, starts = pl.pallas_call(
        gather,
        name="gather",
        out_shape=[jax.ShapeDtypeStruct((windows, *page), F32)] * 2,
        in_specs=[smem, smem, vmem, vmem],
        out_specs=[vmem, vmem],
    )(centers, batch_of, padded, probes)

    terms = pl.pallas_call(
        functools.partial(chain, windows, group, groups),
        name="chain",
        out_shape=jax.ShapeDtypeStruct((windows, *page), F32),
        in_specs=[vmem, vmem, vmem, vmem, vmem],
        out_specs=vmem,
        scratch_shapes=[
            pltpu.VMEM((group, 8, 2 * n), F32),
            pltpu.VMEM((group + 1, 2 * n, 2 * n), BF16),
            pltpu.VMEM((group + 1, 2 * n, 2 * n), BF16),
            pltpu.VMEM((group + 1, 2 * n, 2 * n), BF16),
            pltpu.VMEM((group + 1, 2 * n, 2 * n), BF16),
            pltpu.VMEM((most, group, *page), F32),
            pltpu.VMEM((most, group, *page), F32),
            pltpu.VMEM((most, *page), F32),
            pltpu.VMEM((most, *page), F32),
            pltpu.VMEM((most, *page), F32),
            pltpu.VMEM((most, *page), F32),
            pltpu.VMEM((windows, *page), F32),
            dma((group,)),
            dma((group,)),
            dma((windows,)),
            dma((most, group)),
            dma((most,)),
            dma((most,)),
            dma((most,)),
            dma((most,)),
            dma((most, group)),
            dma((windows,)),
        ],
        compiler_params=pltpu.CompilerParams(collective_id=0, has_side_effects=True),
    )(phase, tables, cuts, starts, measured)

    total = pl.pallas_call(
        spread,
        name="spread",
        out_shape=wide_shape,
        in_specs=[smem, vmem],
        out_specs=vmem,
    )(centers, terms)

    result = pl.pallas_call(
        fold,
        name="fold",
        out_shape=tile_shape,
        in_specs=[vmem],
        out_specs=vmem,
        scratch_shapes=edges,
        compiler_params=pltpu.CompilerParams(collective_id=2, has_side_effects=True),
    )(total)
    return result[None]


def solution(mesh):
    placed = (
        P("depth", None, "tx", "ty"),
        P("depth"),
        P(),
        P("tx", "ty", None, None),
        P("tx", "ty", None, None),
        P("tx", "ty", None, None, None),
    )
    return jax.shard_map(
        local, mesh=mesh, in_specs=placed, out_specs=P("depth", None, "tx", "ty"), check_vma=False
    )
```

```python
import functools
import math

import jax
import jax.numpy as jnp
from jax import lax
from jax.experimental import pallas as pl
from jax.experimental.pallas import tpu as pltpu
from jax.sharding import PartitionSpec as P

LAG = 13
MESH = pl.DeviceIdType.MESH
F32 = jnp.float32
BF16 = jnp.bfloat16


SIDES = [(dx, dy) for dx in (-1, 0, 1) for dy in (-1, 0, 1) if dx or dy]


def around(dx, dy):
    tx, ty = lax.axis_size("tx"), lax.axis_size("ty")
    return {
        "tx": lax.rem(lax.axis_index("tx") + dx + tx, tx),
        "ty": lax.rem(lax.axis_index("ty") + dy + ty, ty),
    }


def greet_all(more=0):
    barrier = pltpu.get_barrier_semaphore()
    for dx, dy in SIDES:
        pl.semaphore_signal(barrier, inc=1, device_id=around(dx, dy), device_id_type=MESH)
    pl.semaphore_wait(barrier, len(SIDES) + more)


def packed(first, second, upper):
    n = first.shape[-1]
    lane = lax.broadcasted_iota(jnp.int32, first.shape, 1)
    keep = lane >= n // 2 if upper else lane < n // 2
    return jnp.where(keep, first, pltpu.roll(second, n // 2, 1))


def exchange(strips, pages, corners, strips_in, pages_in, corners_in, sent, got):
    copies = []
    for k, (dx, dy) in enumerate(SIDES):
        if dy == 0:
            src, dst = strips[dx], strips_in.at[(dx + 1) // 2]
        elif dx == 0:
            src, dst = pages.at[(dy + 1) // 2], pages_in.at[(dy + 1) // 2]
        else:
            at = (dx + 1) + (dy + 1) // 2
            src, dst = corners.at[at], corners_in.at[at]
        copies.append(
            pltpu.make_async_remote_copy(
                src_ref=src, dst_ref=dst, send_sem=sent.at[k], recv_sem=got.at[k],
                device_id=around(dx, dy), device_id_type=MESH,
            )
        )
    return copies


def pack_sides(source, rows, columns, pages, corners):
    for dy in (-1, 1):
        upper, cols = columns[dy]
        first, count = rows[0]
        half = count // 2
        for plane in range(2):
            pages[(dy + 1) // 2, plane] = packed(
                source[plane, first : first + half, cols], source[plane, first + half : first + count, cols], upper
            )
        for dx in (-1, 1):
            first, count = rows[dx]
            corners[(dx + 1) + (dy + 1) // 2] = packed(
                source[0, first : first + count, cols], source[1, first : first + count, cols], upper
            )


def enlarge(
    tile, phase, padded, phases, pages, corners, strips_in, pages_in, corners_in, sent, got, phase_in, phase_sems
):
    side, n = tile.shape[1], tile.shape[1] // 2
    half = n // 2
    place = lax.axis_index("depth")
    mine = lax.rem(place, 2)
    partner = {"depth": place + 1 - 2 * mine}
    pl.semaphore_signal(pltpu.get_barrier_semaphore(), inc=1, device_id=partner, device_id_type=MESH)
    greet_all(1)
    rows = {-1: (0, half), 0: (0, side), 1: (side - half, half)}
    columns = {-1: (False, slice(0, n)), 1: (True, slice(side - n, side))}
    strips = {-1: tile.at[:, pl.ds(0, half), :], 1: tile.at[:, pl.ds(side - half, half), :]}
    copies = exchange(strips, pages, corners, strips_in, pages_in, corners_in, sent, got)
    for copy, (dx, dy) in zip(copies, SIDES):
        if dy == 0:
            copy.start()
    swap = pltpu.make_async_remote_copy(
        src_ref=phase, dst_ref=phase_in, send_sem=phase_sems.at[0], recv_sem=phase_sems.at[1],
        device_id=partner, device_id_type=MESH,
    )
    swap.start()
    pack_sides(tile, rows, columns, pages, corners)
    for copy, (dx, dy) in zip(copies, SIDES):
        if dy != 0:
            copy.start()
    padded[:, half : half + side, n : n + side] = tile[...]
    target_rows = {-1: slice(half + side, side + n), 1: slice(0, half)}
    target_cols = {-1: slice(n + side, 2 * n + side), 1: slice(0, n)}
    for copy, (dx, dy) in zip(copies, SIDES):
        copy.wait_recv()
        if dy == 0:
            padded[:, target_rows[dx], n : n + side] = strips_in[(dx + 1) // 2]
        elif dx == 0:
            for plane in range(2):
                page = pages_in[(dy + 1) // 2, plane]
                padded[plane, half : half + n, target_cols[dy]] = page
                padded[plane, half + n : half + side, target_cols[dy]] = pltpu.roll(page, half, 1)
        else:
            corner = corners_in[(dx + 1) + (dy + 1) // 2]
            padded[0, target_rows[dx], target_cols[dy]] = corner
            padded[1, target_rows[dx], target_cols[dy]] = pltpu.roll(corner, half, 1)
    swap.wait_recv()
    phases[mine] = phase[...]
    phases[1 - mine] = phase_in[...]
    swap.wait_send()
    for copy in copies:
        copy.wait_send()


def fold(total, result, pages, corners, strips_in, pages_in, corners_in, sent, got):
    side, n = result.shape[1], result.shape[1] // 2
    half = n // 2
    greet_all()
    rows = {-1: (0, half), 0: (half, side), 1: (half + side, half)}
    columns = {-1: (True, slice(0, n)), 1: (False, slice(n + side, 2 * n + side))}
    mid = pl.ds(n, side)
    strips = {-1: total.at[:, pl.ds(0, half), mid], 1: total.at[:, pl.ds(half + side, half), mid]}
    copies = exchange(strips, pages, corners, strips_in, pages_in, corners_in, sent, got)
    for copy, (dx, dy) in zip(copies, SIDES):
        if dy == 0:
            copy.start()
    pack_sides(total, rows, columns, pages, corners)
    for copy, (dx, dy) in zip(copies, SIDES):
        if dy != 0:
            copy.start()
    result[...] = total[:, half : half + side, n : n + side]
    target_rows = {-1: slice(side - half, side), 1: slice(0, half)}
    target_cols = {-1: slice(side - n, side), 1: slice(0, n)}

    def masked(page, dy):
        lane = lax.broadcasted_iota(jnp.int32, page.shape, 1)
        return jnp.where(lane >= half if dy == -1 else lane < half, page, 0.0)

    for copy, (dx, dy) in zip(copies, SIDES):
        copy.wait_recv()
        if dy == 0:
            result[:, target_rows[dx], :] += strips_in[(dx + 1) // 2]
        elif dx == 0:
            for plane in range(2):
                page = pages_in[(dy + 1) // 2, plane]
                result[plane, 0:n, target_cols[dy]] += masked(page, dy)
                result[plane, n:side, target_cols[dy]] += masked(pltpu.roll(page, half, 1), dy)
        else:
            corner = corners_in[(dx + 1) + (dy + 1) // 2]
            result[0, target_rows[dx], target_cols[dy]] += masked(corner, dy)
            result[1, target_rows[dx], target_cols[dy]] += masked(pltpu.roll(corner, half, 1), dy)
    for copy in copies:
        copy.wait_send()


def split(values):
    high = values.astype(BF16)
    return high, (values - high.astype(F32)).astype(BF16)


def times(wave, high_table, low_table):
    high, low = split(wave)
    total = jnp.dot(high, low_table, preferred_element_type=F32)
    total += jnp.dot(low, high_table, preferred_element_type=F32)
    return total + jnp.dot(high, high_table, preferred_element_type=F32)


def turned(wave):
    n = wave.shape[0]
    return jnp.concatenate([wave[:, :n].T, wave[:, n:].T], axis=1)


def both_sides(wave, high_table, low_table):
    return times(turned(times(wave, high_table, low_table)), high_table, low_table)


def multiply(first, second):
    n = first.shape[0]
    a, b, c, d = first[:, :n], first[:, n:], second[:, :n], second[:, n:]
    return jnp.concatenate([a * c - b * d, a * d + b * c], axis=1)


def conj_multiply(first, second):
    n = first.shape[0]
    a, b, c, d = first[:, :n], first[:, n:], second[:, :n], second[:, n:]
    return jnp.concatenate([a * c + b * d, a * d - b * c], axis=1)


def keep_table(real, imag, at, high_ref, low_ref):
    n = real.shape[0]
    (rh, rl), (ih, il) = split(real), split(imag)
    for ref, r, m in ((high_ref, rh, ih), (low_ref, rl, il)):
        ref[at, 0:n, 0:n] = r
        ref[at, 0:n, n : 2 * n] = m
        ref[at, n : 2 * n, 0:n] = -m
        ref[at, n : 2 * n, n : 2 * n] = r


def gather(centers, owners, padded, probes, cuts, starts):
    windows, n = cuts.shape[:2]
    flipped = lax.rem(lax.axis_index("depth"), 2) == 0

    @pl.loop(0, windows)
    def _(w):
        row, col = centers[0, 0, 0, w], centers[0, 0, 1, w] + n // 2
        row_in, col_in = lax.rem(row, 8), lax.rem(col, 128)
        rows = pl.ds(pl.multiple_of(row - row_in, 8), n + 8)
        cols = pl.ds(pl.multiple_of(col - col_in, 128), 2 * n)
        planes = []
        for plane in range(2):
            block = padded[plane, rows, cols]
            block = pltpu.roll(block, lax.rem(2 * n - col_in, 2 * n), 1)[:, :n]
            planes.append(pltpu.roll(block, lax.rem(n + 8 - row_in, n + 8), 0)[:n])

        @pl.when(flipped)
        def _():
            cuts[w] = jnp.concatenate([planes[0].T, planes[1].T], axis=1)

        @pl.when(jnp.logical_not(flipped))
        def _():
            cuts[w] = jnp.concatenate(planes, axis=1)

        probe = probes[owners[0, 0, 0, w]]
        starts[w] = jnp.concatenate([probe[0], probe[1]], axis=1)


def chain(
    windows, stages,
    phases, tables, cut, starts, measured,
    terms,
    forth_high, forth_low, back_high, back_low,
    other, psis, turned_terms, waves_in, waves_out, turns_in, turns_out,
    patch_sent, patch_got, wave_sent, wave_got, turn_sent, turn_got, term_sent, term_got,
):
    n = tables.shape[0]
    place = lax.axis_index("depth")
    home = lax.rem(place, 2) == 0
    stage = lax.div(place, 2)
    last = stages - 1
    partner = jnp.where(home, place + 1, place - 1)
    before = home & (stage > 0)
    after = home & (stage < last)

    def copy(src, dst, sent, got, target):
        return pltpu.make_async_remote_copy(
            src_ref=src, dst_ref=dst, send_sem=sent, recv_sem=got,
            device_id={"depth": target}, device_id_type=MESH,
        )

    def patch_copy(w):
        return copy(cut.at[w], other.at[w], patch_sent.at[w], patch_got.at[w], partner)

    def wave_copy(j):
        return copy(waves_out.at[j], waves_in.at[j], wave_sent.at[j], wave_got.at[j], place + 2)

    def turn_copy(j):
        return copy(turns_out.at[j], turns_in.at[j], turn_sent.at[j], turn_got.at[j], place - 2)

    def term_copy(j):
        return copy(turned_terms.at[j], terms.at[j], term_sent.at[j], term_got.at[j], partner)

    barrier = pltpu.get_barrier_semaphore()
    pl.semaphore_signal(barrier, inc=1, device_id={"depth": partner}, device_id_type=MESH)

    @pl.when(before)
    def _():
        pl.semaphore_signal(barrier, inc=1, device_id={"depth": place - 2}, device_id_type=MESH)

    @pl.when(after)
    def _():
        pl.semaphore_signal(barrier, inc=1, device_id={"depth": place + 2}, device_id_type=MESH)

    pl.semaphore_wait(barrier, 1 + jnp.where(before, 1, 0) + jnp.where(after, 1, 0))

    @pl.when(jnp.logical_not(home))
    def _():
        @pl.loop(0, windows)
        def _(w):
            patch_copy(w).start()

    @pl.when(home)
    def _():
        cosine, sine = tables[:, :n], tables[:, n:]
        keep_table(cosine, -sine, 2, forth_high, forth_low)
        keep_table(cosine, sine, 2, back_high, back_low)
        for r in range(2):
            real, imag = phases[r, 0:1, :n], phases[r, 0:1, n:]
            scaled = jnp.concatenate([cosine * real - sine * imag, cosine * imag + sine * real], axis=1)
            table = times(scaled, forth_high[2], forth_low[2])
            keep_table(table[:, :n], table[:, n:], r, forth_high, forth_low)
            keep_table(table[:, :n], -table[:, n:], r, back_high, back_low)

    def forth(wave, at):
        return both_sides(wave, forth_high[at], forth_low[at])

    def back(wave, at):
        return both_sides(wave, back_high[at], back_low[at])

    def through(j):
        first = forth(waves_in[j], 0)
        psis[0, j] = first
        second = forth(multiply(first, cut[j]), 1)
        psis[1, j] = second
        return multiply(second, other[j])

    def detect(j, wave):
        far = forth(wave, 2)
        real, imag = far[:, :n], far[:, n:]
        excess = 2.0 * (real * real + imag * imag - measured[j].T)
        turns_in[j] = back(jnp.concatenate([excess * real, excess * imag], axis=1), 2)

    def second_term(j):
        turned_terms[j] = conj_multiply(psis[1, j], turns_in[j])

    def first_back(j):
        return back(conj_multiply(other[j], turns_in[j]), 1)

    def first_term(j, wave):
        terms[j] = turned(conj_multiply(psis[0, j], wave))

    def second_back(j, wave):
        turns_out[j] = back(conj_multiply(cut[j], wave), 0)

    @pl.when(after)
    def _():
        lag = jnp.minimum(windows, lax.div((2 * (last - stage) + 1) * LAG, 7))

        @pl.loop(0, windows + lag)
        def _(t):
            @pl.when(t < windows)
            def _():
                patch_copy(t).wait_recv()

                @pl.when(stage == 0)
                def _():
                    waves_in[t] = starts[t]

                @pl.when(stage > 0)
                def _():
                    wave_copy(t).wait_recv()

                waves_out[t] = through(t)
                wave_copy(t).start()

            @pl.when(t >= lag)
            def _():
                j = t - lag
                turn_copy(j).wait_recv()

                @pl.when(stage == 0)
                def _():
                    second_term(j)
                    term_copy(j).start()
                    first_term(j, first_back(j))

                @pl.when(stage > 0)
                def _():
                    wave = first_back(j)
                    second_back(j, wave)
                    turn_copy(j).start()
                    second_term(j)
                    first_term(j, wave)

                    @pl.when(t >= windows)
                    def _():
                        term_copy(j).start()

        @pl.when(stage > 0)
        def _():
            @pl.loop(0, windows - lag)
            def _(j):
                term_copy(j).start()

    @pl.when(home & (stage == last))
    def _():
        def arrive(t):
            patch_copy(t).wait_recv()
            wave_copy(t).wait_recv()

        def leave(t):
            turn_copy(t).start()
            term_copy(t).start()

        def finish(t):
            wave = first_back(t)
            second_term(t)
            second_back(t, wave)
            first_term(t, wave)

        arrive(0)
        detect(0, through(0))

        @pl.loop(1, windows)
        def _(t):
            arrive(t)
            finish(t - 1)
            detect(t, through(t))
            leave(t - 1)

        finish(windows - 1)
        leave(windows - 1)

    @pl.when(home)
    def _():
        @pl.loop(0, windows)
        def _(j):
            @pl.when(stage < last)
            def _():
                wave_copy(j).wait_send()

            @pl.when(stage > 0)
            def _():
                turn_copy(j).wait_send()

            term_copy(j).wait_send()

    @pl.when(jnp.logical_not(home))
    def _():
        @pl.loop(0, windows)
        def _(j):
            patch_copy(j).wait_send()
            term_copy(j).wait_recv()


def spread(centers, terms, total):
    windows, n = terms.shape[0], terms.shape[1]
    total[...] = jnp.zeros(total.shape, F32)

    @pl.loop(0, windows)
    def _(w):
        row, col = centers[0, 0, 0, w], centers[0, 0, 1, w] + n // 2
        row_in, col_in = lax.rem(row, 8), lax.rem(col, 128)
        rows = pl.ds(pl.multiple_of(row - row_in, 8), n + 8)
        cols = pl.ds(pl.multiple_of(col - col_in, 128), 2 * n)
        term = terms[w]
        for plane in range(2):
            block = term[:, plane * n : (plane + 1) * n]
            block = jnp.concatenate([block, jnp.zeros((8, n), F32)], axis=0)
            block = pltpu.roll(block, row_in, 0)
            block = jnp.concatenate([block, jnp.zeros((n + 8, n), F32)], axis=1)
            total[plane, rows, cols] += pltpu.roll(block, col_in, 1)


def local(slices, thickness, probes, centers, batch_of, intensity):
    sections = lax.axis_size("depth")
    n = probes.shape[-1]
    half = n // 2
    measured = intensity[0, 0]
    windows = measured.shape[0]
    places = jnp.transpose(centers, (0, 1, 3, 2))
    owners = jnp.transpose(batch_of, (0, 1, 3, 2))
    counts = jnp.arange(n, dtype=jnp.int32)
    angles = (counts[:, None] * counts[None, :] % n).astype(F32) * (2.0 * math.pi / n)
    tables = jnp.concatenate([jnp.cos(angles), jnp.sin(angles)], axis=1) * (1.0 / math.sqrt(n))
    offset = (counts + half) % n - half
    turn = thickness[0] * ((offset * offset).astype(F32) * (math.pi / (half * half)))
    turn = jnp.broadcast_to(turn[None], (8, n))
    phase = jnp.concatenate([jnp.cos(turn), -jnp.sin(turn)], axis=1)

    smem = pl.BlockSpec(memory_space=pltpu.SMEM)
    vmem = pl.BlockSpec(memory_space=pltpu.VMEM)
    page = (n, 2 * n)
    dma = pltpu.SemaphoreType.DMA
    side = slices.shape[2]
    tile_shape = jax.ShapeDtypeStruct((2, side, side), F32)
    wide_shape = jax.ShapeDtypeStruct((2, side + n, side + 2 * n), F32)
    edges = [
        pltpu.VMEM((2, 2, n, n), F32),
        pltpu.VMEM((4, half, n), F32),
        pltpu.VMEM((2, 2, half, side), F32),
        pltpu.VMEM((2, 2, n, n), F32),
        pltpu.VMEM((4, half, n), F32),
        dma((len(SIDES),)),
        dma((len(SIDES),)),
    ]
    padded, phases = pl.pallas_call(
        enlarge,
        name="enlarge",
        out_shape=[wide_shape, jax.ShapeDtypeStruct((2, 8, 2 * n), F32)],
        in_specs=[vmem, vmem],
        out_specs=[vmem, vmem],
        scratch_shapes=[*edges, pltpu.VMEM((8, 2 * n), F32), dma((2,))],
        compiler_params=pltpu.CompilerParams(collective_id=1, has_side_effects=True),
    )(slices[0], phase)

    cuts, starts = pl.pallas_call(
        gather,
        name="gather",
        out_shape=[jax.ShapeDtypeStruct((windows, *page), F32)] * 2,
        in_specs=[smem, smem, vmem, vmem],
        out_specs=[vmem, vmem],
    )(places, owners, padded, probes)

    terms = pl.pallas_call(
        functools.partial(chain, windows, sections // 2),
        name="chain",
        out_shape=jax.ShapeDtypeStruct((windows, *page), F32),
        in_specs=[vmem] * 5,
        out_specs=vmem,
        scratch_shapes=[pltpu.VMEM((3, 2 * n, 2 * n), BF16)] * 4
        + [pltpu.VMEM((windows, *page), F32), pltpu.VMEM((2, windows, *page), F32)]
        + [pltpu.VMEM((windows, *page), F32)] * 5
        + [dma((windows,))] * 8,
        compiler_params=pltpu.CompilerParams(collective_id=0, has_side_effects=True),
    )(phases, tables, cuts, starts, measured)

    total = pl.pallas_call(
        spread,
        name="spread",
        out_shape=wide_shape,
        in_specs=[smem, vmem],
        out_specs=vmem,
    )(places, terms)

    result = pl.pallas_call(
        fold,
        name="fold",
        out_shape=tile_shape,
        in_specs=[vmem],
        out_specs=vmem,
        scratch_shapes=edges,
        compiler_params=pltpu.CompilerParams(collective_id=2, has_side_effects=True),
    )(total)
    return result[None]


def solution(mesh):
    placed = (
        P("depth", None, "tx", "ty"),
        P("depth"),
        P(),
        P("tx", "ty", None, None),
        P("tx", "ty", None, None),
        P("tx", "ty", None, None, None),
    )
    return jax.shard_map(
        local, mesh=mesh, in_specs=placed, out_specs=P("depth", None, "tx", "ty"), check_vma=False
    )
```

```python
import functools
import math

import jax
import jax.numpy as jnp
from jax import lax
from jax.experimental import pallas as pl
from jax.experimental.pallas import tpu as pltpu
from jax.sharding import PartitionSpec as P

LAG = 13
MESH = pl.DeviceIdType.MESH
F32 = jnp.float32
BF16 = jnp.bfloat16


SIDES = [(dx, dy) for dx in (-1, 0, 1) for dy in (-1, 0, 1) if dx or dy]


def around(dx, dy):
    tx, ty = lax.axis_size("tx"), lax.axis_size("ty")
    return {
        "tx": lax.rem(lax.axis_index("tx") + dx + tx, tx),
        "ty": lax.rem(lax.axis_index("ty") + dy + ty, ty),
    }


def greet_all(more=0):
    barrier = pltpu.get_barrier_semaphore()
    for dx, dy in SIDES:
        pl.semaphore_signal(barrier, inc=1, device_id=around(dx, dy), device_id_type=MESH)
    pl.semaphore_wait(barrier, len(SIDES) + more)


def packed(first, second, upper):
    n = first.shape[-1]
    lane = lax.broadcasted_iota(jnp.int32, first.shape, 1)
    keep = lane >= n // 2 if upper else lane < n // 2
    return jnp.where(keep, first, pltpu.roll(second, n // 2, 1))


def exchange(strips, pages, corners, strips_in, pages_in, corners_in, sent, got):
    copies = []
    for k, (dx, dy) in enumerate(SIDES):
        if dy == 0:
            src, dst = strips[dx], strips_in.at[(dx + 1) // 2]
        elif dx == 0:
            src, dst = pages.at[(dy + 1) // 2], pages_in.at[(dy + 1) // 2]
        else:
            at = (dx + 1) + (dy + 1) // 2
            src, dst = corners.at[at], corners_in.at[at]
        copies.append(
            pltpu.make_async_remote_copy(
                src_ref=src, dst_ref=dst, send_sem=sent.at[k], recv_sem=got.at[k],
                device_id=around(dx, dy), device_id_type=MESH,
            )
        )
    return copies


def pack_sides(source, rows, columns, pages, corners):
    for dy in (-1, 1):
        upper, cols = columns[dy]
        first, count = rows[0]
        half = count // 2
        for plane in range(2):
            pages[(dy + 1) // 2, plane] = packed(
                source[plane, first : first + half, cols], source[plane, first + half : first + count, cols], upper
            )
        for dx in (-1, 1):
            first, count = rows[dx]
            corners[(dx + 1) + (dy + 1) // 2] = packed(
                source[0, first : first + count, cols], source[1, first : first + count, cols], upper
            )


def enlarge(
    tile, phase, padded, phases, pages, corners, strips_in, pages_in, corners_in, sent, got, phase_in, phase_sems
):
    side, n = tile.shape[1], tile.shape[1] // 2
    half = n // 2
    place = lax.axis_index("depth")
    mine = lax.rem(place, 2)
    partner = {"depth": place + 1 - 2 * mine}
    pl.semaphore_signal(pltpu.get_barrier_semaphore(), inc=1, device_id=partner, device_id_type=MESH)
    greet_all(1)
    rows = {-1: (0, half), 0: (0, side), 1: (side - half, half)}
    columns = {-1: (False, slice(0, n)), 1: (True, slice(side - n, side))}
    strips = {-1: tile.at[:, pl.ds(0, half), :], 1: tile.at[:, pl.ds(side - half, half), :]}
    copies = exchange(strips, pages, corners, strips_in, pages_in, corners_in, sent, got)
    for copy, (dx, dy) in zip(copies, SIDES):
        if dy == 0:
            copy.start()
    swap = pltpu.make_async_remote_copy(
        src_ref=phase, dst_ref=phase_in, send_sem=phase_sems.at[0], recv_sem=phase_sems.at[1],
        device_id=partner, device_id_type=MESH,
    )
    swap.start()
    pack_sides(tile, rows, columns, pages, corners)
    for copy, (dx, dy) in zip(copies, SIDES):
        if dy != 0:
            copy.start()
    padded[:, half : half + side, n : n + side] = tile[...]
    target_rows = {-1: slice(half + side, side + n), 1: slice(0, half)}
    target_cols = {-1: slice(n + side, 2 * n + side), 1: slice(0, n)}
    for copy, (dx, dy) in zip(copies, SIDES):
        copy.wait_recv()
        if dy == 0:
            padded[:, target_rows[dx], n : n + side] = strips_in[(dx + 1) // 2]
        elif dx == 0:
            for plane in range(2):
                page = pages_in[(dy + 1) // 2, plane]
                padded[plane, half : half + n, target_cols[dy]] = page
                padded[plane, half + n : half + side, target_cols[dy]] = pltpu.roll(page, half, 1)
        else:
            corner = corners_in[(dx + 1) + (dy + 1) // 2]
            padded[0, target_rows[dx], target_cols[dy]] = corner
            padded[1, target_rows[dx], target_cols[dy]] = pltpu.roll(corner, half, 1)
    swap.wait_recv()
    phases[mine] = phase[...]
    phases[1 - mine] = phase_in[...]
    swap.wait_send()
    for copy in copies:
        copy.wait_send()


def fold(total, result, pages, corners, strips_in, pages_in, corners_in, sent, got):
    side, n = result.shape[1], result.shape[1] // 2
    half = n // 2
    greet_all()
    rows = {-1: (0, half), 0: (half, side), 1: (half + side, half)}
    columns = {-1: (True, slice(0, n)), 1: (False, slice(n + side, 2 * n + side))}
    mid = pl.ds(n, side)
    strips = {-1: total.at[:, pl.ds(0, half), mid], 1: total.at[:, pl.ds(half + side, half), mid]}
    copies = exchange(strips, pages, corners, strips_in, pages_in, corners_in, sent, got)
    for copy, (dx, dy) in zip(copies, SIDES):
        if dy == 0:
            copy.start()
    pack_sides(total, rows, columns, pages, corners)
    for copy, (dx, dy) in zip(copies, SIDES):
        if dy != 0:
            copy.start()
    result[...] = total[:, half : half + side, n : n + side]
    target_rows = {-1: slice(side - half, side), 1: slice(0, half)}
    target_cols = {-1: slice(side - n, side), 1: slice(0, n)}

    def masked(page, dy):
        lane = lax.broadcasted_iota(jnp.int32, page.shape, 1)
        return jnp.where(lane >= half if dy == -1 else lane < half, page, 0.0)

    for copy, (dx, dy) in zip(copies, SIDES):
        copy.wait_recv()
        if dy == 0:
            result[:, target_rows[dx], :] += strips_in[(dx + 1) // 2]
        elif dx == 0:
            for plane in range(2):
                page = pages_in[(dy + 1) // 2, plane]
                result[plane, 0:n, target_cols[dy]] += masked(page, dy)
                result[plane, n:side, target_cols[dy]] += masked(pltpu.roll(page, half, 1), dy)
        else:
            corner = corners_in[(dx + 1) + (dy + 1) // 2]
            result[0, target_rows[dx], target_cols[dy]] += masked(corner, dy)
            result[1, target_rows[dx], target_cols[dy]] += masked(pltpu.roll(corner, half, 1), dy)
    for copy in copies:
        copy.wait_send()


def split(values):
    high = values.astype(BF16)
    return high, (values - high.astype(F32)).astype(BF16)


def times(wave, high_table, low_table):
    high, low = split(wave)
    total = jnp.dot(high, low_table, preferred_element_type=F32)
    total += jnp.dot(low, high_table, preferred_element_type=F32)
    return total + jnp.dot(high, high_table, preferred_element_type=F32)


def turned(wave):
    n = wave.shape[0]
    return jnp.concatenate([wave[:, :n].T, wave[:, n:].T], axis=1)


def both_sides(wave, high_table, low_table):
    return times(turned(times(wave, high_table, low_table)), high_table, low_table)


def multiply(first, second):
    n = first.shape[0]
    a, b, c, d = first[:, :n], first[:, n:], second[:, :n], second[:, n:]
    return jnp.concatenate([a * c - b * d, a * d + b * c], axis=1)


def conj_multiply(first, second):
    n = first.shape[0]
    a, b, c, d = first[:, :n], first[:, n:], second[:, :n], second[:, n:]
    return jnp.concatenate([a * c + b * d, a * d - b * c], axis=1)


def keep_table(real, imag, at, high_ref, low_ref):
    n = real.shape[0]
    (rh, rl), (ih, il) = split(real), split(imag)
    for ref, r, m in ((high_ref, rh, ih), (low_ref, rl, il)):
        ref[at, 0:n, 0:n] = r
        ref[at, 0:n, n : 2 * n] = m
        ref[at, n : 2 * n, 0:n] = -m
        ref[at, n : 2 * n, n : 2 * n] = r


def gather(places, owners, padded, first_probe, second_probe, cuts, starts):
    n = cuts.shape[1]
    flipped = lax.rem(lax.axis_index("depth"), 2) == 0
    patches = []
    for k in range(2):
        w = 2 * pl.program_id(0) + k
        row, col = places[0, w], places[1, w] + n // 2
        row_in, col_in = lax.rem(row, 8), lax.rem(col, n)
        rows = pl.ds(pl.multiple_of(row - row_in, 8), n + 8)
        cols = pl.ds(pl.multiple_of(col - col_in, n), 2 * n)
        for plane in range(2):
            block = pltpu.roll(padded[plane, rows, cols], lax.rem(2 * n - col_in, 2 * n), 1)[:, :n]
            patches.append(pltpu.roll(block, lax.rem(n + 8 - row_in, n + 8), 0)[:n])
    for k, probe in enumerate((first_probe, second_probe)):
        starts[k] = jnp.concatenate([probe[0, 0], probe[0, 1]], axis=1)

    @pl.when(flipped)
    def _():
        for k in range(2):
            cuts[k] = jnp.concatenate([patches[2 * k].T, patches[2 * k + 1].T], axis=1)

    @pl.when(jnp.logical_not(flipped))
    def _():
        for k in range(2):
            cuts[k] = jnp.concatenate(patches[2 * k : 2 * k + 2], axis=1)


def chain(
    windows, stages,
    phases, tables, cut, starts, measured,
    terms,
    forth_high, forth_low, back_high, back_low,
    other, psis, turned_terms, waves_in, waves_out, turns_in, turns_out, targets,
    patch_sent, patch_got, wave_sent, wave_got, turn_sent, turn_got, term_sent, term_got,
    start_got, target_got,
):
    n = tables.shape[0]
    place = lax.axis_index("depth")
    home = lax.rem(place, 2) == 0
    stage = lax.div(place, 2)
    last = stages - 1
    partner = jnp.where(home, place + 1, place - 1)
    before = home & (stage > 0)
    after = home & (stage < last)

    def copy(src, dst, sent, got, target):
        return pltpu.make_async_remote_copy(
            src_ref=src, dst_ref=dst, send_sem=sent, recv_sem=got,
            device_id={"depth": target}, device_id_type=MESH,
        )

    def patch_copy(w):
        return copy(cut.at[w], other.at[w], patch_sent.at[w], patch_got.at[w], partner)

    def wave_copy(j):
        return copy(waves_out.at[j], waves_in.at[j], wave_sent.at[j], wave_got.at[j], place + 2)

    def turn_copy(j):
        return copy(turns_out.at[j], turns_in.at[j], turn_sent.at[j], turn_got.at[j], place - 2)

    def term_copy(j):
        return copy(turned_terms.at[j], terms.at[j], term_sent.at[j], term_got.at[j], partner)

    barrier = pltpu.get_barrier_semaphore()
    pl.semaphore_signal(barrier, inc=1, device_id={"depth": partner}, device_id_type=MESH)

    @pl.when(before)
    def _():
        pl.semaphore_signal(barrier, inc=1, device_id={"depth": place - 2}, device_id_type=MESH)

    @pl.when(after)
    def _():
        pl.semaphore_signal(barrier, inc=1, device_id={"depth": place + 2}, device_id_type=MESH)

    def start_copy(j):
        return pltpu.make_async_copy(starts.at[j], waves_in.at[j], start_got.at[j])

    def target_copy(j):
        return pltpu.make_async_copy(measured.at[j], targets.at[j], target_got.at[j])

    @pl.when(home & (stage == 0))
    def _():
        @pl.loop(0, windows)
        def _(j):
            start_copy(j).start()

    @pl.when(home & (stage == last))
    def _():
        @pl.loop(0, windows)
        def _(j):
            target_copy(j).start()

    @pl.when(home)
    def _():
        cosine, sine = tables[:, :n], tables[:, n:]
        keep_table(cosine, -sine, 2, forth_high, forth_low)
        keep_table(cosine, sine, 2, back_high, back_low)
        for r in range(2):
            real, imag = phases[r, 0:1, :n], phases[r, 0:1, n:]
            scaled = jnp.concatenate([cosine * real - sine * imag, cosine * imag + sine * real], axis=1)
            table = times(scaled, forth_high[2], forth_low[2])
            keep_table(table[:, :n], table[:, n:], r, forth_high, forth_low)
            keep_table(table[:, :n], -table[:, n:], r, back_high, back_low)

    pl.semaphore_wait(barrier, 1 + jnp.where(before, 1, 0) + jnp.where(after, 1, 0))

    @pl.when(jnp.logical_not(home))
    def _():
        @pl.loop(0, windows)
        def _(w):
            patch_copy(w).start()

    def forth(wave, at):
        return both_sides(wave, forth_high[at], forth_low[at])

    def back(wave, at):
        return both_sides(wave, back_high[at], back_low[at])

    def through(j):
        first = forth(waves_in[j], 0)
        psis[0, j] = first
        second = forth(multiply(first, cut[j]), 1)
        psis[1, j] = second
        return multiply(second, other[j])

    def detect(j, wave):
        far = forth(wave, 2)
        real, imag = far[:, :n], far[:, n:]
        excess = 2.0 * (real * real + imag * imag - targets[j].T)
        turns_in[j] = back(jnp.concatenate([excess * real, excess * imag], axis=1), 2)

    def second_term(j):
        turned_terms[j] = conj_multiply(psis[1, j], turns_in[j])

    def first_back(j):
        return back(conj_multiply(other[j], turns_in[j]), 1)

    def first_term(j, wave):
        terms[j] = turned(conj_multiply(psis[0, j], wave))

    def second_back(j, wave):
        turns_out[j] = back(conj_multiply(cut[j], wave), 0)

    @pl.when(after)
    def _():
        lag = jnp.minimum(windows, lax.div((2 * (last - stage) + 1) * LAG, 7))

        @pl.loop(0, windows + lag)
        def _(t):
            @pl.when(t < windows)
            def _():
                patch_copy(t).wait_recv()

                @pl.when(stage == 0)
                def _():
                    start_copy(t).wait()

                @pl.when(stage > 0)
                def _():
                    wave_copy(t).wait_recv()

                waves_out[t] = through(t)
                wave_copy(t).start()

            @pl.when(t >= lag)
            def _():
                j = t - lag
                turn_copy(j).wait_recv()

                @pl.when(stage == 0)
                def _():
                    second_term(j)
                    term_copy(j).start()
                    first_term(j, first_back(j))

                @pl.when(stage > 0)
                def _():
                    wave = first_back(j)
                    second_back(j, wave)
                    turn_copy(j).start()
                    second_term(j)
                    first_term(j, wave)

                    @pl.when(t >= windows)
                    def _():
                        term_copy(j).start()

        @pl.when(stage > 0)
        def _():
            @pl.loop(0, windows - lag)
            def _(j):
                term_copy(j).start()

    @pl.when(home & (stage == last))
    def _():
        def arrive(t):
            target_copy(t).wait()
            patch_copy(t).wait_recv()
            wave_copy(t).wait_recv()

        def leave(t):
            turn_copy(t).start()
            term_copy(t).start()

        def finish(t):
            wave = first_back(t)
            second_term(t)
            second_back(t, wave)
            first_term(t, wave)

        arrive(0)
        detect(0, through(0))

        @pl.loop(1, windows)
        def _(t):
            arrive(t)
            finish(t - 1)
            detect(t, through(t))
            leave(t - 1)

        finish(windows - 1)
        leave(windows - 1)

    @pl.when(home)
    def _():
        @pl.loop(0, windows)
        def _(j):
            @pl.when(stage < last)
            def _():
                wave_copy(j).wait_send()

            @pl.when(stage > 0)
            def _():
                turn_copy(j).wait_send()

            term_copy(j).wait_send()

    @pl.when(jnp.logical_not(home))
    def _():
        @pl.loop(0, windows)
        def _(j):
            patch_copy(j).wait_send()
            term_copy(j).wait_recv()


def spread(centers, terms, total):
    windows, n = terms.shape[0], terms.shape[1]
    total[...] = jnp.zeros(total.shape, F32)

    @pl.loop(0, windows)
    def _(w):
        row, col = centers[0, w], centers[1, w] + n // 2
        row_in, col_in = lax.rem(row, 8), lax.rem(col, 128)
        rows = pl.ds(pl.multiple_of(row - row_in, 8), n + 8)
        cols = pl.ds(pl.multiple_of(col - col_in, 128), 2 * n)
        term = terms[w]
        for plane in range(2):
            block = term[:, plane * n : (plane + 1) * n]
            block = jnp.concatenate([block, jnp.zeros((8, n), F32)], axis=0)
            block = pltpu.roll(block, row_in, 0)
            block = jnp.concatenate([block, jnp.zeros((n + 8, n), F32)], axis=1)
            total[plane, rows, cols] += pltpu.roll(block, col_in, 1)


def local(slices, thickness, probes, centers, batch_of, intensity):
    sections = lax.axis_size("depth")
    n = probes.shape[-1]
    half = n // 2
    measured = intensity[0, 0]
    windows = measured.shape[0]
    places = jnp.transpose(centers, (0, 1, 3, 2))[0, 0]
    owners = jnp.transpose(batch_of, (0, 1, 3, 2))[0, 0]
    counts = jnp.arange(n, dtype=jnp.int32)
    angles = (counts[:, None] * counts[None, :] % n).astype(F32) * (2.0 * math.pi / n)
    tables = jnp.concatenate([jnp.cos(angles), jnp.sin(angles)], axis=1) * (1.0 / math.sqrt(n))
    offset = (counts + half) % n - half
    turn = thickness[0] * ((offset * offset).astype(F32) * (math.pi / (half * half)))
    turn = jnp.broadcast_to(turn[None], (8, n))
    phase = jnp.concatenate([jnp.cos(turn), -jnp.sin(turn)], axis=1)

    smem = pl.BlockSpec(memory_space=pltpu.SMEM)
    vmem = pl.BlockSpec(memory_space=pltpu.VMEM)
    stay = pl.BlockSpec(memory_space=pl.ANY)
    page = (n, 2 * n)
    dma = pltpu.SemaphoreType.DMA
    side = slices.shape[2]
    tile_shape = jax.ShapeDtypeStruct((2, side, side), F32)
    wide_shape = jax.ShapeDtypeStruct((2, side + n, side + 2 * n), F32)
    edges = [
        pltpu.VMEM((2, 2, n, n), F32),
        pltpu.VMEM((4, half, n), F32),
        pltpu.VMEM((2, 2, half, side), F32),
        pltpu.VMEM((2, 2, n, n), F32),
        pltpu.VMEM((4, half, n), F32),
        dma((len(SIDES),)),
        dma((len(SIDES),)),
    ]
    padded, phases = pl.pallas_call(
        enlarge,
        name="enlarge",
        out_shape=[wide_shape, jax.ShapeDtypeStruct((2, 8, 2 * n), F32)],
        in_specs=[vmem, vmem],
        out_specs=[vmem, vmem],
        scratch_shapes=[*edges, pltpu.VMEM((8, 2 * n), F32), dma((2,))],
        compiler_params=pltpu.CompilerParams(collective_id=1, has_side_effects=True),
    )(slices[0], phase)

    probe_page = (1, 2, n, n)
    pair = pl.BlockSpec((2, *page), lambda p, c, o: (p, 0, 0))
    cuts, starts = pl.pallas_call(
        gather,
        name="gather",
        out_shape=[jax.ShapeDtypeStruct((windows, *page), F32)] * 2,
        grid_spec=pltpu.PrefetchScalarGridSpec(
            num_scalar_prefetch=2,
            grid=(windows // 2,),
            in_specs=[
                pl.BlockSpec(wide_shape.shape, lambda p, c, o: (0, 0, 0), pipeline_mode=pl.Buffered(1)),
                pl.BlockSpec(probe_page, lambda p, c, o: (o[0, 2 * p], 0, 0, 0)),
                pl.BlockSpec(probe_page, lambda p, c, o: (o[0, 2 * p + 1], 0, 0, 0)),
            ],
            out_specs=[pair, pair],
        ),
    )(places, owners, padded, probes, probes)

    terms = pl.pallas_call(
        functools.partial(chain, windows, sections // 2),
        name="chain",
        out_shape=jax.ShapeDtypeStruct((windows, *page), F32),
        in_specs=[vmem, vmem, vmem, stay, stay],
        out_specs=vmem,
        scratch_shapes=[pltpu.VMEM((3, 2 * n, 2 * n), BF16)] * 4
        + [pltpu.VMEM((windows, *page), F32), pltpu.VMEM((2, windows, *page), F32)]
        + [pltpu.VMEM((windows, *page), F32)] * 5
        + [pltpu.VMEM((windows, n, n), F32)]
        + [dma((windows,))] * 10,
        compiler_params=pltpu.CompilerParams(collective_id=0, has_side_effects=True),
    )(phases, tables, cuts, starts, measured)

    total = pl.pallas_call(
        spread,
        name="spread",
        out_shape=wide_shape,
        in_specs=[smem, vmem],
        out_specs=vmem,
    )(places, terms)

    result = pl.pallas_call(
        fold,
        name="fold",
        out_shape=tile_shape,
        in_specs=[vmem],
        out_specs=vmem,
        scratch_shapes=edges,
        compiler_params=pltpu.CompilerParams(collective_id=2, has_side_effects=True),
    )(total)
    return result[None]


def solution(mesh):
    placed = (
        P("depth", None, "tx", "ty"),
        P("depth"),
        P(),
        P("tx", "ty", None, None),
        P("tx", "ty", None, None),
        P("tx", "ty", None, None, None),
    )
    return jax.shard_map(
        local, mesh=mesh, in_specs=placed, out_specs=P("depth", None, "tx", "ty"), check_vma=False
    )
```

```python
import functools
import math

import jax
import jax.numpy as jnp
from jax import lax
from jax.experimental import pallas as pl
from jax.experimental.pallas import tpu as pltpu
from jax.sharding import PartitionSpec as P

LAG = 13
MESH = pl.DeviceIdType.MESH
F32 = jnp.float32
BF16 = jnp.bfloat16


SIDES = [(dx, dy) for dx in (-1, 0, 1) for dy in (-1, 0, 1) if dx or dy]


def around(dx, dy):
    tx, ty = lax.axis_size("tx"), lax.axis_size("ty")
    return {
        "tx": lax.rem(lax.axis_index("tx") + dx + tx, tx),
        "ty": lax.rem(lax.axis_index("ty") + dy + ty, ty),
    }


def greet_all(more=0):
    barrier = pltpu.get_barrier_semaphore()
    for dx, dy in SIDES:
        pl.semaphore_signal(barrier, inc=1, device_id=around(dx, dy), device_id_type=MESH)
    pl.semaphore_wait(barrier, len(SIDES) + more)


def packed(first, second, upper):
    n = first.shape[-1]
    lane = lax.broadcasted_iota(jnp.int32, first.shape, 1)
    keep = lane >= n // 2 if upper else lane < n // 2
    return jnp.where(keep, first, pltpu.roll(second, n // 2, 1))


def exchange(strips, pages, corners, strips_in, pages_in, corners_in, sent, got):
    copies = []
    for k, (dx, dy) in enumerate(SIDES):
        if dy == 0:
            src, dst = strips[dx], strips_in.at[(dx + 1) // 2]
        elif dx == 0:
            src, dst = pages.at[(dy + 1) // 2], pages_in.at[(dy + 1) // 2]
        else:
            at = (dx + 1) + (dy + 1) // 2
            src, dst = corners.at[at], corners_in.at[at]
        copies.append(
            pltpu.make_async_remote_copy(
                src_ref=src, dst_ref=dst, send_sem=sent.at[k], recv_sem=got.at[k],
                device_id=around(dx, dy), device_id_type=MESH,
            )
        )
    return copies


def pack_sides(source, rows, columns, pages, corners):
    for dy in (-1, 1):
        upper, cols = columns[dy]
        first, count = rows[0]
        half = count // 2
        for plane in range(2):
            pages[(dy + 1) // 2, plane] = packed(
                source[plane, first : first + half, cols], source[plane, first + half : first + count, cols], upper
            )
        for dx in (-1, 1):
            first, count = rows[dx]
            corners[(dx + 1) + (dy + 1) // 2] = packed(
                source[0, first : first + count, cols], source[1, first : first + count, cols], upper
            )


def enlarge(
    tile, phase, padded, phases, pages, corners, strips_in, pages_in, corners_in, sent, got, phase_in, phase_sems
):
    side, n = tile.shape[1], tile.shape[1] // 2
    half = n // 2
    place = lax.axis_index("depth")
    mine = lax.rem(place, 2)
    partner = {"depth": place + 1 - 2 * mine}
    pl.semaphore_signal(pltpu.get_barrier_semaphore(), inc=1, device_id=partner, device_id_type=MESH)
    greet_all(1)
    rows = {-1: (0, half), 0: (0, side), 1: (side - half, half)}
    columns = {-1: (False, slice(0, n)), 1: (True, slice(side - n, side))}
    strips = {-1: tile.at[:, pl.ds(0, half), :], 1: tile.at[:, pl.ds(side - half, half), :]}
    copies = exchange(strips, pages, corners, strips_in, pages_in, corners_in, sent, got)
    for copy, (dx, dy) in zip(copies, SIDES):
        if dy == 0:
            copy.start()
    swap = pltpu.make_async_remote_copy(
        src_ref=phase, dst_ref=phase_in, send_sem=phase_sems.at[0], recv_sem=phase_sems.at[1],
        device_id=partner, device_id_type=MESH,
    )
    swap.start()
    pack_sides(tile, rows, columns, pages, corners)
    for copy, (dx, dy) in zip(copies, SIDES):
        if dy != 0:
            copy.start()
    padded[:, half : half + side, n : n + side] = tile[...]
    target_rows = {-1: slice(half + side, side + n), 1: slice(0, half)}
    target_cols = {-1: slice(n + side, 2 * n + side), 1: slice(0, n)}
    for copy, (dx, dy) in zip(copies, SIDES):
        copy.wait_recv()
        if dy == 0:
            padded[:, target_rows[dx], n : n + side] = strips_in[(dx + 1) // 2]
        elif dx == 0:
            for plane in range(2):
                page = pages_in[(dy + 1) // 2, plane]
                padded[plane, half : half + n, target_cols[dy]] = page
                padded[plane, half + n : half + side, target_cols[dy]] = pltpu.roll(page, half, 1)
        else:
            corner = corners_in[(dx + 1) + (dy + 1) // 2]
            padded[0, target_rows[dx], target_cols[dy]] = corner
            padded[1, target_rows[dx], target_cols[dy]] = pltpu.roll(corner, half, 1)
    swap.wait_recv()
    phases[mine] = phase[...]
    phases[1 - mine] = phase_in[...]
    swap.wait_send()
    for copy in copies:
        copy.wait_send()


def fold(total, result, pages, corners, strips_in, pages_in, corners_in, sent, got):
    side, n = result.shape[1], result.shape[1] // 2
    half = n // 2
    greet_all()
    rows = {-1: (0, half), 0: (half, side), 1: (half + side, half)}
    columns = {-1: (True, slice(0, n)), 1: (False, slice(n + side, 2 * n + side))}
    mid = pl.ds(n, side)
    strips = {-1: total.at[:, pl.ds(0, half), mid], 1: total.at[:, pl.ds(half + side, half), mid]}
    copies = exchange(strips, pages, corners, strips_in, pages_in, corners_in, sent, got)
    for copy, (dx, dy) in zip(copies, SIDES):
        if dy == 0:
            copy.start()
    pack_sides(total, rows, columns, pages, corners)
    for copy, (dx, dy) in zip(copies, SIDES):
        if dy != 0:
            copy.start()
    result[...] = total[:, half : half + side, n : n + side]
    target_rows = {-1: slice(side - half, side), 1: slice(0, half)}
    target_cols = {-1: slice(side - n, side), 1: slice(0, n)}

    def masked(page, dy):
        lane = lax.broadcasted_iota(jnp.int32, page.shape, 1)
        return jnp.where(lane >= half if dy == -1 else lane < half, page, 0.0)

    for copy, (dx, dy) in zip(copies, SIDES):
        copy.wait_recv()
        if dy == 0:
            result[:, target_rows[dx], :] += strips_in[(dx + 1) // 2]
        elif dx == 0:
            for plane in range(2):
                page = pages_in[(dy + 1) // 2, plane]
                result[plane, 0:n, target_cols[dy]] += masked(page, dy)
                result[plane, n:side, target_cols[dy]] += masked(pltpu.roll(page, half, 1), dy)
        else:
            corner = corners_in[(dx + 1) + (dy + 1) // 2]
            result[0, target_rows[dx], target_cols[dy]] += masked(corner, dy)
            result[1, target_rows[dx], target_cols[dy]] += masked(pltpu.roll(corner, half, 1), dy)
    for copy in copies:
        copy.wait_send()


def split(values):
    high = values.astype(BF16)
    return high, (values - high.astype(F32)).astype(BF16)


def times(wave, high_table, low_table):
    high, low = split(wave)
    total = jnp.dot(high, low_table, preferred_element_type=F32)
    total += jnp.dot(low, high_table, preferred_element_type=F32)
    return total + jnp.dot(high, high_table, preferred_element_type=F32)


def turned(wave):
    n = wave.shape[0]
    return jnp.concatenate([wave[:, :n].T, wave[:, n:].T], axis=1)


def both_sides(wave, high_table, low_table):
    return times(turned(times(wave, high_table, low_table)), high_table, low_table)


def multiply(first, second):
    n = first.shape[0]
    a, b, c, d = first[:, :n], first[:, n:], second[:, :n], second[:, n:]
    return jnp.concatenate([a * c - b * d, a * d + b * c], axis=1)


def conj_multiply(first, second):
    n = first.shape[0]
    a, b, c, d = first[:, :n], first[:, n:], second[:, :n], second[:, n:]
    return jnp.concatenate([a * c + b * d, a * d - b * c], axis=1)


def keep_table(real, imag, at, high_ref, low_ref):
    n = real.shape[0]
    (rh, rl), (ih, il) = split(real), split(imag)
    for ref, r, m in ((high_ref, rh, ih), (low_ref, rl, il)):
        ref[at, 0:n, 0:n] = r
        ref[at, 0:n, n : 2 * n] = m
        ref[at, n : 2 * n, 0:n] = -m
        ref[at, n : 2 * n, n : 2 * n] = r


def gather(centers, owners, padded, probes, cuts, starts):
    windows, n = cuts.shape[:2]
    flipped = lax.rem(lax.axis_index("depth"), 2) == 0

    @pl.loop(0, windows // 2)
    def _(p):
        patches = []
        for k in range(2):
            w = 2 * p + k
            row, col = centers[0, 0, 0, w], centers[0, 0, 1, w] + n // 2
            row_in, col_in = lax.rem(row, 8), lax.rem(col, 128)
            rows = pl.ds(pl.multiple_of(row - row_in, 8), n + 8)
            cols = pl.ds(pl.multiple_of(col - col_in, 128), 2 * n)
            for plane in range(2):
                block = pltpu.roll(padded[plane, rows, cols], lax.rem(2 * n - col_in, 2 * n), 1)[:, :n]
                patches.append(pltpu.roll(block, lax.rem(n + 8 - row_in, n + 8), 0)[:n])
            probe = probes[owners[0, 0, 0, w]]
            starts[w] = jnp.concatenate([probe[0], probe[1]], axis=1)

        @pl.when(flipped)
        def _():
            for k in range(2):
                cuts[2 * p + k] = jnp.concatenate([patches[2 * k].T, patches[2 * k + 1].T], axis=1)

        @pl.when(jnp.logical_not(flipped))
        def _():
            for k in range(2):
                cuts[2 * p + k] = jnp.concatenate(patches[2 * k : 2 * k + 2], axis=1)


def chain(
    windows, stages,
    phases, tables, cut, starts, measured,
    terms,
    forth_high, forth_low, back_high, back_low,
    other, psis, turned_terms, waves_in, waves_out, turns_in, turns_out,
    patch_sent, patch_got, wave_sent, wave_got, turn_sent, turn_got, term_sent, term_got,
):
    n = tables.shape[0]
    place = lax.axis_index("depth")
    home = lax.rem(place, 2) == 0
    stage = lax.div(place, 2)
    last = stages - 1
    partner = jnp.where(home, place + 1, place - 1)
    before = home & (stage > 0)
    after = home & (stage < last)

    def copy(src, dst, sent, got, target):
        return pltpu.make_async_remote_copy(
            src_ref=src, dst_ref=dst, send_sem=sent, recv_sem=got,
            device_id={"depth": target}, device_id_type=MESH,
        )

    def patch_copy(w):
        return copy(cut.at[w], other.at[w], patch_sent.at[w], patch_got.at[w], partner)

    def wave_copy(j):
        return copy(waves_out.at[j], waves_in.at[j], wave_sent.at[j], wave_got.at[j], place + 2)

    def turn_copy(j):
        return copy(turns_out.at[j], turns_in.at[j], turn_sent.at[j], turn_got.at[j], place - 2)

    def term_copy(j):
        return copy(turned_terms.at[j], terms.at[j], term_sent.at[j], term_got.at[j], partner)

    barrier = pltpu.get_barrier_semaphore()
    pl.semaphore_signal(barrier, inc=1, device_id={"depth": partner}, device_id_type=MESH)

    @pl.when(before)
    def _():
        pl.semaphore_signal(barrier, inc=1, device_id={"depth": place - 2}, device_id_type=MESH)

    @pl.when(after)
    def _():
        pl.semaphore_signal(barrier, inc=1, device_id={"depth": place + 2}, device_id_type=MESH)

    pl.semaphore_wait(barrier, 1 + jnp.where(before, 1, 0) + jnp.where(after, 1, 0))

    @pl.when(jnp.logical_not(home))
    def _():
        @pl.loop(0, windows)
        def _(w):
            patch_copy(w).start()

    @pl.when(home)
    def _():
        cosine, sine = tables[:, :n], tables[:, n:]
        keep_table(cosine, -sine, 2, forth_high, forth_low)
        keep_table(cosine, sine, 2, back_high, back_low)
        for r in range(2):
            real, imag = phases[r, 0:1, :n], phases[r, 0:1, n:]
            scaled = jnp.concatenate([cosine * real - sine * imag, cosine * imag + sine * real], axis=1)
            table = times(scaled, forth_high[2], forth_low[2])
            keep_table(table[:, :n], table[:, n:], r, forth_high, forth_low)
            keep_table(table[:, :n], -table[:, n:], r, back_high, back_low)

    def forth(wave, at):
        return both_sides(wave, forth_high[at], forth_low[at])

    def back(wave, at):
        return both_sides(wave, back_high[at], back_low[at])

    def through(j):
        first = forth(waves_in[j], 0)
        psis[0, j] = first
        second = forth(multiply(first, cut[j]), 1)
        psis[1, j] = second
        return multiply(second, other[j])

    def detect(j, wave):
        far = forth(wave, 2)
        real, imag = far[:, :n], far[:, n:]
        excess = 2.0 * (real * real + imag * imag - measured[j].T)
        turns_in[j] = back(jnp.concatenate([excess * real, excess * imag], axis=1), 2)

    def second_term(j):
        turned_terms[j] = conj_multiply(psis[1, j], turns_in[j])

    def first_back(j):
        return back(conj_multiply(other[j], turns_in[j]), 1)

    def first_term(j, wave):
        terms[j] = turned(conj_multiply(psis[0, j], wave))

    def second_back(j, wave):
        turns_out[j] = back(conj_multiply(cut[j], wave), 0)

    @pl.when(after)
    def _():
        lag = jnp.minimum(windows, lax.div((2 * (last - stage) + 1) * LAG, 7))

        @pl.loop(0, windows + lag)
        def _(t):
            @pl.when(t < windows)
            def _():
                patch_copy(t).wait_recv()

                @pl.when(stage == 0)
                def _():
                    waves_in[t] = starts[t]

                @pl.when(stage > 0)
                def _():
                    wave_copy(t).wait_recv()

                waves_out[t] = through(t)
                wave_copy(t).start()

            @pl.when(t >= lag)
            def _():
                j = t - lag
                turn_copy(j).wait_recv()

                @pl.when(stage == 0)
                def _():
                    second_term(j)
                    term_copy(j).start()
                    first_term(j, first_back(j))

                @pl.when(stage > 0)
                def _():
                    wave = first_back(j)
                    second_back(j, wave)
                    turn_copy(j).start()
                    second_term(j)
                    first_term(j, wave)

                    @pl.when(t >= windows)
                    def _():
                        term_copy(j).start()

        @pl.when(stage > 0)
        def _():
            @pl.loop(0, windows - lag)
            def _(j):
                term_copy(j).start()

    @pl.when(home & (stage == last))
    def _():
        def arrive(t):
            patch_copy(t).wait_recv()
            wave_copy(t).wait_recv()

        def leave(t):
            turn_copy(t).start()
            term_copy(t).start()

        def finish(t):
            wave = first_back(t)
            second_term(t)
            second_back(t, wave)
            first_term(t, wave)

        arrive(0)
        detect(0, through(0))

        @pl.loop(1, windows)
        def _(t):
            arrive(t)
            finish(t - 1)
            detect(t, through(t))
            leave(t - 1)

        finish(windows - 1)
        leave(windows - 1)

    @pl.when(home)
    def _():
        @pl.loop(0, windows)
        def _(j):
            @pl.when(stage < last)
            def _():
                wave_copy(j).wait_send()

            @pl.when(stage > 0)
            def _():
                turn_copy(j).wait_send()

            term_copy(j).wait_send()

    @pl.when(jnp.logical_not(home))
    def _():
        @pl.loop(0, windows)
        def _(j):
            patch_copy(j).wait_send()
            term_copy(j).wait_recv()


def spread(centers, terms, total):
    windows, n = terms.shape[0], terms.shape[1]
    total[...] = jnp.zeros(total.shape, F32)

    @pl.loop(0, windows // 2)
    def _(p):
        for plane in range(2):
            adds = []
            for k in range(2):
                w = 2 * p + k
                row, col = centers[0, 0, 0, w], centers[0, 0, 1, w] + n // 2
                row_in, col_in = lax.rem(row, 8), lax.rem(col, 128)
                rows = pl.ds(pl.multiple_of(row - row_in, 8), n + 8)
                cols = pl.ds(pl.multiple_of(col - col_in, 128), 2 * n)
                block = jnp.concatenate([terms[w, :, plane * n : (plane + 1) * n], jnp.zeros((8, n), F32)], axis=0)
                block = jnp.concatenate([pltpu.roll(block, row_in, 0), jnp.zeros((n + 8, n), F32)], axis=1)
                adds.append((rows, cols, pltpu.roll(block, col_in, 1)))
            for rows, cols, block in adds:
                total[plane, rows, cols] += block


def local(slices, thickness, probes, centers, batch_of, intensity):
    sections = lax.axis_size("depth")
    n = probes.shape[-1]
    half = n // 2
    measured = intensity[0, 0]
    windows = measured.shape[0]
    places = jnp.transpose(centers, (0, 1, 3, 2))
    owners = jnp.transpose(batch_of, (0, 1, 3, 2))
    counts = jnp.arange(n, dtype=jnp.int32)
    angles = (counts[:, None] * counts[None, :] % n).astype(F32) * (2.0 * math.pi / n)
    tables = jnp.concatenate([jnp.cos(angles), jnp.sin(angles)], axis=1) * (1.0 / math.sqrt(n))
    offset = (counts + half) % n - half
    turn = thickness[0] * ((offset * offset).astype(F32) * (math.pi / (half * half)))
    turn = jnp.broadcast_to(turn[None], (8, n))
    phase = jnp.concatenate([jnp.cos(turn), -jnp.sin(turn)], axis=1)

    smem = pl.BlockSpec(memory_space=pltpu.SMEM)
    vmem = pl.BlockSpec(memory_space=pltpu.VMEM)
    page = (n, 2 * n)
    dma = pltpu.SemaphoreType.DMA
    side = slices.shape[2]
    tile_shape = jax.ShapeDtypeStruct((2, side, side), F32)
    wide_shape = jax.ShapeDtypeStruct((2, side + n, side + 2 * n), F32)
    edges = [
        pltpu.VMEM((2, 2, n, n), F32),
        pltpu.VMEM((4, half, n), F32),
        pltpu.VMEM((2, 2, half, side), F32),
        pltpu.VMEM((2, 2, n, n), F32),
        pltpu.VMEM((4, half, n), F32),
        dma((len(SIDES),)),
        dma((len(SIDES),)),
    ]
    padded, phases = pl.pallas_call(
        enlarge,
        name="enlarge",
        out_shape=[wide_shape, jax.ShapeDtypeStruct((2, 8, 2 * n), F32)],
        in_specs=[vmem, vmem],
        out_specs=[vmem, vmem],
        scratch_shapes=[*edges, pltpu.VMEM((8, 2 * n), F32), dma((2,))],
        compiler_params=pltpu.CompilerParams(collective_id=1, has_side_effects=True),
    )(slices[0], phase)

    cuts, starts = pl.pallas_call(
        gather,
        name="gather",
        out_shape=[jax.ShapeDtypeStruct((windows, *page), F32)] * 2,
        in_specs=[smem, smem, vmem, vmem],
        out_specs=[vmem, vmem],
    )(places, owners, padded, probes)

    terms = pl.pallas_call(
        functools.partial(chain, windows, sections // 2),
        name="chain",
        out_shape=jax.ShapeDtypeStruct((windows, *page), F32),
        in_specs=[vmem] * 5,
        out_specs=vmem,
        scratch_shapes=[pltpu.VMEM((3, 2 * n, 2 * n), BF16)] * 4
        + [pltpu.VMEM((windows, *page), F32), pltpu.VMEM((2, windows, *page), F32)]
        + [pltpu.VMEM((windows, *page), F32)] * 5
        + [dma((windows,))] * 8,
        compiler_params=pltpu.CompilerParams(collective_id=0, has_side_effects=True),
    )(phases, tables, cuts, starts, measured)

    total = pl.pallas_call(
        spread,
        name="spread",
        out_shape=wide_shape,
        in_specs=[smem, vmem],
        out_specs=vmem,
    )(places, terms)

    result = pl.pallas_call(
        fold,
        name="fold",
        out_shape=tile_shape,
        in_specs=[vmem],
        out_specs=vmem,
        scratch_shapes=edges,
        compiler_params=pltpu.CompilerParams(collective_id=2, has_side_effects=True),
    )(total)
    return result[None]


def solution(mesh):
    placed = (
        P("depth", None, "tx", "ty"),
        P("depth"),
        P(),
        P("tx", "ty", None, None),
        P("tx", "ty", None, None),
        P("tx", "ty", None, None, None),
    )
    return jax.shard_map(
        local, mesh=mesh, in_specs=placed, out_specs=P("depth", None, "tx", "ty"), check_vma=False
    )
```
